32 devices in a mesh: dp: 2 (over x), tp: 4 (over z), cp: 4 (over y, core).
Axes of the slice: x: 2, y: 2, z: 4, core: 2. Of those that a mesh axis runs over, the one named last changes fastest.
Arguments:
- tokens_in: bfloat16 [12288, 3584], P(('dp', 'cp', 'tp')), parts along dimension 0
- grad_out: bfloat16 [12288, 3584], P(('dp', 'cp', 'tp')), parts along dimension 0
- w_query: bfloat16 [3584, 3584], P(None, 'tp')
- w_key: bfloat16 [3584, 512], P(None, 'tp')
- w_value: bfloat16 [3584, 512], P(None, 'tp')
- w_out: bfloat16 [3584, 3584], P('tp')
Outputs:
- output 1: bfloat16 [12288, 3584], P(('dp', 'cp', 'tp')), parts along dimension 0
- output 2: bfloat16 [12288, 3584], P(('dp', 'cp', 'tp')), parts along dimension 0
There are 2 independent parts. The reference program is written for one: setup_inputs(seed, part) draws one part's arguments, and reference() takes and returns one part's arrays. A program takes and returns all parts, laid end to end along the dimension named above; an argument that names none is the same for every part.
All inputs are finite; a program needn't handle non-finite values.
Results may differ from the reference program's by a relative error of at most 0.00951519.
Values are sent between devices in bfloat16 or wider.
A program may use at most 1 GiB of HBM per device.

```python
import math
import jax
import jax.numpy as jnp
from jax import lax

D = 3584
HQ = 28
HKV = 4
HEAD = 128
CP = 4
SEQ = 6144

GROUP_SIZE = HQ // HKV
SEQ_LOC = SEQ // CP
PIECE = SEQ_LOC // 2
ROW_BLOCK = 2 ** max(3, min(7, int(math.log2(max(1, 2 ** 22 // (SEQ * HQ))))))


def setup_inputs(seed: int = 0, part: int = 0) -> dict:
    base_key = jax.random.key(seed)
    data_key, weight_key = jax.random.split(base_key)
    part_key = jax.random.fold_in(data_key, part)
    key_x, key_dy = jax.random.split(part_key)
    key_q, key_k, key_v, key_o = jax.random.split(weight_key, 4)
    query_gain = math.sqrt(0.5 * math.log(SEQ))
    tokens_in = jax.random.normal(key_x, (SEQ, D), jnp.float32).astype(jnp.bfloat16)
    grad_out = jax.random.normal(key_dy, (SEQ, D), jnp.float32).astype(jnp.bfloat16)
    w_query = (jax.random.normal(key_q, (D, HQ * HEAD), jnp.float32) * (query_gain / math.sqrt(D))).astype(jnp.bfloat16)
    w_key = (jax.random.normal(key_k, (D, HKV * HEAD), jnp.float32) / math.sqrt(D)).astype(jnp.bfloat16)
    w_value = (jax.random.normal(key_v, (D, HKV * HEAD), jnp.float32) / math.sqrt(D)).astype(jnp.bfloat16)
    w_out = (jax.random.normal(key_o, (HQ * HEAD, D), jnp.float32) / math.sqrt(HQ * HEAD)).astype(jnp.bfloat16)
    return dict(tokens_in=tokens_in, grad_out=grad_out, w_query=w_query, w_key=w_key, w_value=w_value, w_out=w_out)


def fold_positions():
    row_ids = jnp.arange(SEQ, dtype=jnp.int32)
    shard_idx = row_ids // SEQ_LOC
    within = row_ids % SEQ_LOC
    piece_id = jnp.where(within < PIECE, shard_idx, 2 * CP - 1 - shard_idx)
    return piece_id * PIECE + within % PIECE


def reference(tokens_in, grad_out, w_query, w_key, w_value, w_out):
    score_scale = HEAD ** -0.5
    positions = fold_positions()
    queries = jnp.dot(tokens_in, w_query, preferred_element_type=jnp.float32).astype(jnp.bfloat16).reshape(SEQ, HKV, GROUP_SIZE, HEAD)
    keys_all = jnp.dot(tokens_in, w_key, preferred_element_type=jnp.float32).astype(jnp.bfloat16).reshape(SEQ, HKV, HEAD)
    values_all = jnp.dot(tokens_in, w_value, preferred_element_type=jnp.float32).astype(jnp.bfloat16).reshape(SEQ, HKV, HEAD)
    d_out = jnp.dot(grad_out, w_out.T, preferred_element_type=jnp.float32).astype(jnp.bfloat16).reshape(SEQ, HKV, GROUP_SIZE, HEAD)
    keys_f32 = keys_all.astype(jnp.float32)
    values_f32 = values_all.astype(jnp.float32)
    block_count = SEQ // ROW_BLOCK

    def block_step(acc_pair, blk_in):
        dk_acc, dv_acc = acc_pair
        q_blk, do_blk, pos_blk = blk_in
        query_f32 = q_blk.astype(jnp.float32)
        dout_f32 = do_blk.astype(jnp.float32)
        scores = jnp.einsum('qhgd,khd->hgqk', query_f32, keys_f32) * score_scale
        allowed = pos_blk[:, None] >= positions[None, :]
        scores = jnp.where(allowed, scores, -jnp.inf)
        log_norm = jax.nn.logsumexp(scores, axis=-1, keepdims=True)
        prob_f32 = jnp.exp(scores - log_norm).astype(jnp.bfloat16).astype(jnp.float32)
        out_blk = jnp.einsum('hgqk,khd->qhgd', prob_f32, values_f32).astype(jnp.bfloat16)
        row_delta = jnp.sum(dout_f32 * out_blk.astype(jnp.float32), axis=-1)
        d_prob = jnp.einsum('qhgd,khd->hgqk', dout_f32, values_f32)
        dscore_f32 = (prob_f32 * (d_prob - jnp.transpose(row_delta, (1, 2, 0))[..., None])).astype(jnp.bfloat16).astype(jnp.float32)
        dq_blk = (jnp.einsum('hgqk,khd->qhgd', dscore_f32, keys_f32) * score_scale).astype(jnp.bfloat16)
        dk_acc = dk_acc + jnp.einsum('hgqk,qhgd->khd', dscore_f32, query_f32) * score_scale
        dv_acc = dv_acc + jnp.einsum('hgqk,qhgd->khd', prob_f32, dout_f32)
        return (dk_acc, dv_acc), (out_blk, dq_blk)

    blk_inputs = (queries.reshape(block_count, ROW_BLOCK, HKV, GROUP_SIZE, HEAD), d_out.reshape(block_count, ROW_BLOCK, HKV, GROUP_SIZE, HEAD), positions.reshape(block_count, ROW_BLOCK))
    zeros_kv = jnp.zeros((SEQ, HKV, HEAD), jnp.float32)
    (dk_sum, dv_sum), (out_blocks, dq_blocks) = lax.scan(block_step, (zeros_kv, zeros_kv), blk_inputs)
    attn_out = out_blocks.reshape(SEQ, HQ * HEAD)
    d_query = dq_blocks.reshape(SEQ, HQ * HEAD)
    layer_out = jnp.dot(attn_out, w_out, preferred_element_type=jnp.float32).astype(jnp.bfloat16)
    grad_in = (jnp.dot(d_query, w_query.T, preferred_element_type=jnp.float32)
               + jnp.dot(dk_sum.astype(jnp.bfloat16).reshape(SEQ, HKV * HEAD), w_key.T, preferred_element_type=jnp.float32)
               + jnp.dot(dv_sum.astype(jnp.bfloat16).reshape(SEQ, HKV * HEAD), w_value.T, preferred_element_type=jnp.float32)).astype(jnp.bfloat16)
    return layer_out, grad_in
```

```python
import functools
import jax
import jax.numpy as jnp
from jax import lax
from jax.experimental import pallas as pl
from jax.experimental.pallas import tpu as pltpu
from jax.sharding import PartitionSpec as P

HD = 128
BQ = 256
LOG2E = 1.4426950408889634
SCALE = HD ** -0.5
NT = (((1,), (1,)), ((), ()))
NN = (((1,), (0,)), ((), ()))
NEG = -1e30
VMEM = 60 * 2 ** 20
MESH_ID = pl.DeviceIdType.MESH


def mm(a, b, dims):
    return lax.dot_general(a, b, dims, preferred_element_type=jnp.float32)


def gather_kernel(units, w_ref, out_ref, buf, zs, zr, xs, xr, ys, yr, cs, cr, ls, lo):
    x = lax.axis_index('dp')
    z = lax.axis_index('tp')
    cp = lax.axis_index('cp')
    y = cp // 2
    c = cp % 2
    hz = z // 2
    rows = w_ref.shape[0]
    pr = rows // 8
    ur = pr // units
    dx = (1 - x, z, cp)
    dy = (x, z, (1 - y) * 2 + c)
    dc = (x, z, y * 2 + 1 - c)
    src = [1 - z + 4 * hz, 2 - hz, 3 - 3 * hz]
    bar = pltpu.get_barrier_semaphore()
    for d in [(x, src[0], cp), (x, src[1], cp), (x, src[2], cp), dx, dy, dc]:
        pl.semaphore_signal(bar, inc=1, device_id=d, device_id_type=MESH_ID)
    pl.semaphore_wait(bar, 6)

    def eid(xx, yy, cc):
        return (xx * 2 + yy) * 2 + cc

    def un(s, e, u):
        return out_ref.at[s, pl.ds(pl.multiple_of(e * pr + u * ur, 8), ur), :]

    def rc(a, b, ss, rr, dev):
        return pltpu.make_async_remote_copy(src_ref=a, dst_ref=b, send_sem=ss, recv_sem=rr, device_id=dev,
                                            device_id_type=MESH_ID)

    e0, ex, ey, ed = eid(x, y, c), eid(1 - x, y, c), eid(x, 1 - y, c), eid(1 - x, 1 - y, c)
    zsend = []
    for u in range(units):
        for k in range(3):
            q = rc(w_ref.at[pl.ds(pl.multiple_of(e0 * pr + u * ur, 8), ur), :], un(z, e0, u), zs.at[k, u],
                   zr.at[z, u], (x, src[k], cp))
            q.start()
            zsend.append(q)
    nb = 8
    br = rows // nb

    def inb(i):
        return pltpu.make_async_copy(w_ref.at[pl.ds(i * br, br), :], buf.at[i % 2], ls.at[i % 2])

    def outb(i):
        return pltpu.make_async_copy(buf.at[i % 2], out_ref.at[z, pl.ds(i * br, br), :], lo.at[i % 2])

    inb(0).start()
    for i in range(nb):
        inb(i).wait()
        if i >= 1:
            outb(i - 1).wait()
        if i + 1 < nb:
            inb(i + 1).start()
        outb(i).start()
    outb(nb - 1).wait()

    order = [(u, k) for u in range(units) for k in range(3)]
    n = len(order)
    zrecv, xc, yc, fc, cc = [], [], [], [], []
    for i, (u, k) in enumerate(order):
        s = src[k]
        zrecv.append(rc(un(s, e0, u), un(s, e0, u), zs.at[k, u], zr.at[s, u], (x, s, cp)))
        xc.append(rc(un(s, e0, u), un(s, e0, u), xs.at[i, 0], xr.at[i, 0], dx))
        yc.append(rc(un(s, e0, u), un(s, e0, u), ys.at[i, 0], yr.at[i, 0], dy))
        if i % 2 == 0:
            fc.append(rc(un(s, ex, u), un(s, ex, u), ys.at[i, 1], yr.at[i, 1], dy))
        else:
            fc.append(rc(un(s, ey, u), un(s, ey, u), xs.at[i, 1], xr.at[i, 1], dx))
        cc.append([rc(un(s, e, u), un(s, e, u), cs.at[i, j], cr.at[i, j], dc) for j, e in enumerate((e0, ex, ey, ed))])

    def st1(i):
        zrecv[i].wait_recv()
        first, second = (xc, yc) if i % 2 == 0 else (yc, xc)
        first[i].start()
        second[i].start()
        cc[i][0].start()

    def st2(i):
        first = xc if i % 2 == 0 else yc
        first[i].wait_recv()
        fc[i].start()
        cc[i][1 if i % 2 == 0 else 2].start()

    def st3(i):
        second = yc if i % 2 == 0 else xc
        second[i].wait_recv()
        cc[i][2 if i % 2 == 0 else 1].start()

    def st4(i):
        fc[i].wait_recv()
        cc[i][3].start()

    for i in range(n + 3):
        if i < n:
            st1(i)
        if 0 <= i - 1 < n:
            st2(i - 1)
        if 0 <= i - 2 < n:
            st3(i - 2)
        if 0 <= i - 3 < n:
            st4(i - 3)
    for q in zsend:
        q.wait_send()
    for i in range(n):
        for q in [xc[i], yc[i], fc[i]] + cc[i]:
            q.wait_send()
        for q in cc[i]:
            q.wait_recv()


def gather(w, cid, units):
    rows, cols = w.shape
    dma = pltpu.SemaphoreType.DMA
    n = 3 * units
    return pl.pallas_call(
        functools.partial(gather_kernel, units),
        out_shape=jax.ShapeDtypeStruct((4, rows, cols), w.dtype),
        in_specs=[pl.BlockSpec(memory_space=pltpu.HBM)],
        out_specs=pl.BlockSpec(memory_space=pltpu.HBM),
        scratch_shapes=[pltpu.VMEM((2, rows // 8, cols), w.dtype), dma((3, units)), dma((4, units)), dma((n, 2)),
                        dma((n, 2)), dma((n, 2)), dma((n, 2)), dma((n, 4)), dma((n, 4)), dma((2,)), dma((2,))],
        name=f"gather{cid}",
        compiler_params=pltpu.CompilerParams(collective_id=cid, has_side_effects=True, vmem_limit_bytes=VMEM),
        cost_estimate=pl.CostEstimate(flops=10 ** 11, bytes_accessed=10 ** 7, transcendentals=0))(w)


def qkv_kernel(x_ref, w_ref, q_ref, kv_ref):
    r = mm(x_ref[...], w_ref[0], NN).astype(jnp.bfloat16)
    nq = q_ref.shape[2]
    q_ref[0] = r[:, :nq]
    kv_ref[0] = r[:, nq:]


def qkv_proj(x, wqkv):
    rows, d = x.shape
    ng, _, cols = wqkv.shape
    nq = cols - 2 * HD
    return pl.pallas_call(
        qkv_kernel, grid=(ng,),
        out_shape=[jax.ShapeDtypeStruct((ng, rows, nq), jnp.bfloat16), jax.ShapeDtypeStruct((ng, rows, 2 * HD), jnp.bfloat16)],
        in_specs=[pl.BlockSpec((rows, d), lambda g: (0, 0)), pl.BlockSpec((1, d, cols), lambda g: (g, 0, 0))],
        out_specs=[pl.BlockSpec((1, rows, nq), lambda g: (g, 0, 0)), pl.BlockSpec((1, rows, 2 * HD), lambda g: (g, 0, 0))],
        name="qkv_proj", compiler_params=pltpu.CompilerParams(vmem_limit_bytes=VMEM),
        cost_estimate=pl.CostEstimate(flops=2 * rows * d * cols * ng, bytes_accessed=40 * 10 ** 6, transcendentals=0))(x, wqkv)


def do_kernel(x_ref, w_ref, o_ref):
    o_ref[0] = mm(x_ref[...], w_ref[0], NT).astype(jnp.bfloat16)


def do_proj(dy, wo):
    rows, d = dy.shape
    ng, nq, _ = wo.shape
    return pl.pallas_call(
        do_kernel, grid=(ng,),
        out_shape=jax.ShapeDtypeStruct((ng, rows, nq), jnp.bfloat16),
        in_specs=[pl.BlockSpec((rows, d), lambda g: (0, 0)), pl.BlockSpec((1, nq, d), lambda g: (g, 0, 0))],
        out_specs=pl.BlockSpec((1, rows, nq), lambda g: (g, 0, 0)),
        name="do_proj", compiler_params=pltpu.CompilerParams(vmem_limit_bytes=VMEM),
        cost_estimate=pl.CostEstimate(flops=2 * rows * d * nq * ng, bytes_accessed=30 * 10 ** 6, transcendentals=0))(dy, wo)


def y_kernel(o_ref, w_ref, y_ref):
    acc = mm(o_ref[0], w_ref[0], NN)
    for g in range(1, o_ref.shape[0]):
        acc = acc + mm(o_ref[g], w_ref[g], NN)
    y_ref[...] = acc.astype(jnp.bfloat16)


def y_proj(o, wo):
    ng, rows, nq = o.shape
    d = wo.shape[2]
    bn = 512
    return pl.pallas_call(
        y_kernel, grid=(d // bn,),
        out_shape=jax.ShapeDtypeStruct((rows, d), jnp.bfloat16),
        in_specs=[pl.BlockSpec((ng, rows, nq), lambda j: (0, 0, 0)), pl.BlockSpec((ng, nq, bn), lambda j: (0, 0, j))],
        out_specs=pl.BlockSpec((rows, bn), lambda j: (0, j)),
        name="y_proj", compiler_params=pltpu.CompilerParams(vmem_limit_bytes=VMEM),
        cost_estimate=pl.CostEstimate(flops=2 * rows * d * nq * ng, bytes_accessed=30 * 10 ** 6, transcendentals=0))(o, wo)


def dx_kernel(dq_ref, dkv_ref, w_ref, dx_ref):
    nq = dq_ref.shape[2]
    acc = None
    for g in range(dq_ref.shape[0]):
        t = mm(dq_ref[g], w_ref[g, :, :nq], NT) + mm(dkv_ref[g], w_ref[g, :, nq:], NT)
        acc = t if acc is None else acc + t
    dx_ref[...] = acc.astype(jnp.bfloat16)


def dx_proj(dq, dkv, wqkv):
    ng, rows, nq = dq.shape
    _, d, cols = wqkv.shape
    bn = 512
    return pl.pallas_call(
        dx_kernel, grid=(d // bn,),
        out_shape=jax.ShapeDtypeStruct((rows, d), jnp.bfloat16),
        in_specs=[pl.BlockSpec((ng, rows, nq), lambda j: (0, 0, 0)), pl.BlockSpec((ng, rows, 2 * HD), lambda j: (0, 0, 0)),
                  pl.BlockSpec((ng, bn, cols), lambda j: (0, j, 0))],
        out_specs=pl.BlockSpec((rows, bn), lambda j: (0, j)),
        name="dx_proj", compiler_params=pltpu.CompilerParams(vmem_limit_bytes=VMEM),
        cost_estimate=pl.CostEstimate(flops=2 * rows * d * cols * ng, bytes_accessed=40 * 10 ** 6, transcendentals=0))(dq, dkv, wqkv)


def piece_row(j, piece, n_pieces):
    half = n_pieces // 2
    return jnp.where(j < half, j * 2 * piece, (n_pieces - 1 - j) * 2 * piece + piece)


def key_loop(n, piece, n_pieces, tile):
    per = piece // BQ
    full = n // per

    def whole(j, _):
        tile(pl.multiple_of(piece_row(j, piece, n_pieces), BQ), piece, False)
        return 0

    def part(j, _):
        tile(pl.multiple_of(piece_row(full, piece, n_pieces) + (j - full * per) * BQ, BQ), BQ, False)
        return 0

    lax.fori_loop(0, full, whole, 0)
    lax.fori_loop(full * per, n, part, 0)
    tile(pl.multiple_of(piece_row(full, piece, n_pieces) + (n - full * per) * BQ, BQ), BQ, True)


def keep_mask(size):
    r = lax.broadcasted_iota(jnp.int32, (size, BQ), 0)
    q = lax.broadcasted_iota(jnp.int32, (size, BQ), 1)
    return r <= q


def fwd_kernel(nh, piece, n_pieces, pos_ref, q_ref, kv_ref, o_ref, lse_ref, vt_ref, m_ref, l_ref, acc_ref):
    i = pl.program_id(0)
    n = pos_ref[i]

    @pl.when(i == 0)
    def _():
        for b in range(n_pieces):
            vt_ref[:, b * piece:(b + 1) * piece] = kv_ref[b * piece:(b + 1) * piece, HD:].T

    m_ref[...] = jnp.full_like(m_ref, NEG)
    l_ref[...] = jnp.zeros_like(l_ref)
    acc_ref[...] = jnp.zeros_like(acc_ref)

    def tile(start, size, masked):
        k = kv_ref[pl.ds(start, size), :HD]
        vt = vt_ref[:, pl.ds(start, size)]
        scores = [mm(k, q_ref[:, h * HD:(h + 1) * HD], NT) for h in range(nh)]
        for h in range(nh):
            s = scores[h] * (SCALE * LOG2E)
            if masked:
                s = jnp.where(keep_mask(size), s, NEG)
            m_old = m_ref[h:h + 1, :]
            m_new = jnp.maximum(m_old, jnp.max(s, axis=0, keepdims=True))
            p = jnp.exp2(s - m_new)
            a = jnp.exp2(m_old - m_new)
            m_ref[h:h + 1, :] = m_new
            l_ref[h:h + 1, :] = l_ref[h:h + 1, :] * a + jnp.sum(p, axis=0, keepdims=True)
            o = mm(vt, p.astype(jnp.bfloat16), NN)
            acc_ref[h * HD:(h + 1) * HD, :] = acc_ref[h * HD:(h + 1) * HD, :] * a + o

    key_loop(n, piece, n_pieces, tile)
    for h in range(nh):
        l = l_ref[h:h + 1, :]
        o = acc_ref[h * HD:(h + 1) * HD, :] / l
        o_ref[:, h * HD:(h + 1) * HD] = o.T.astype(jnp.bfloat16)
        lse_ref[0, h:h + 1, :] = m_ref[h:h + 1, :] + jnp.log2(l)


def attn_fwd(pos, q, kv, piece):
    rows, width = q.shape
    nh = width // HD
    keys = kv.shape[0]
    nq = rows // BQ
    gs = pltpu.PrefetchScalarGridSpec(
        num_scalar_prefetch=1, grid=(nq,),
        in_specs=[pl.BlockSpec((BQ, width), lambda i, p: (i, 0)), pl.BlockSpec((keys, 2 * HD), lambda i, p: (0, 0))],
        out_specs=[pl.BlockSpec((BQ, width), lambda i, p: (i, 0)), pl.BlockSpec((1, 8, BQ), lambda i, p: (i, 0, 0))],
        scratch_shapes=[pltpu.VMEM((HD, keys), jnp.bfloat16), pltpu.VMEM((8, BQ), jnp.float32),
                        pltpu.VMEM((8, BQ), jnp.float32), pltpu.VMEM((width, BQ), jnp.float32)])
    return pl.pallas_call(
        functools.partial(fwd_kernel, nh, piece, keys // piece),
        out_shape=[jax.ShapeDtypeStruct(q.shape, jnp.bfloat16), jax.ShapeDtypeStruct((nq, 8, BQ), jnp.float32)],
        grid_spec=gs, name="attn_fwd", compiler_params=pltpu.CompilerParams(vmem_limit_bytes=VMEM),
        cost_estimate=pl.CostEstimate(flops=64 * 10 ** 9, bytes_accessed=10 ** 7, transcendentals=0))(pos, q, kv)


def bwd_kernel(nh, piece, n_pieces, pos_ref, q_ref, do_ref, o_ref, lse_ref, kv_ref, dq_ref, dkv_ref, kt_ref, del_ref, dqt_ref):
    i = pl.program_id(0)
    n = pos_ref[i]

    @pl.when(i == 0)
    def _():
        dkv_ref[...] = jnp.zeros_like(dkv_ref)
        for b in range(n_pieces):
            kt_ref[:, b * piece:(b + 1) * piece] = kv_ref[b * piece:(b + 1) * piece, :HD].T

    for h in range(nh):
        sl = slice(h * HD, (h + 1) * HD)
        pr = do_ref[:, sl].astype(jnp.float32) * o_ref[:, sl].astype(jnp.float32)
        del_ref[h:h + 1, :] = jnp.sum(pr.T, axis=0, keepdims=True)
    dqt_ref[...] = jnp.zeros_like(dqt_ref)

    def tile(start, size, masked):
        for t0 in range(0, size, BQ):
            sub(start + t0, masked)

    def sub(start, masked):
        size = BQ
        k = kv_ref[pl.ds(start, size), :HD]
        v = kv_ref[pl.ds(start, size), HD:]
        kt = kt_ref[:, pl.ds(start, size)]
        dv = None
        dk = None
        for h in range(nh):
            sl = slice(h * HD, (h + 1) * HD)
            s = mm(k, q_ref[:, sl], NT) * (SCALE * LOG2E) - lse_ref[0, h:h + 1, :]
            dp = mm(v, do_ref[:, sl], NT)
            if masked:
                s = jnp.where(keep_mask(size), s, NEG)
            pb = jnp.exp2(s).astype(jnp.bfloat16)
            ds = (pb.astype(jnp.float32) * (dp - del_ref[h:h + 1, :])).astype(jnp.bfloat16)
            dvh = mm(pb, do_ref[:, sl], NN)
            dkh = mm(ds, q_ref[:, sl], NN)
            dv = dvh if dv is None else dv + dvh
            dk = dkh if dk is None else dk + dkh
            dqt_ref[sl, :] += mm(kt, ds, NN)
        dkv_ref[pl.ds(start, size), :HD] += dk * SCALE
        dkv_ref[pl.ds(start, size), HD:] += dv

    key_loop(n, piece, n_pieces, tile)
    for h in range(nh):
        sl = slice(h * HD, (h + 1) * HD)
        dq_ref[:, sl] = (dqt_ref[sl, :] * SCALE).T.astype(jnp.bfloat16)


def attn_bwd(pos, q, do, o, lse, kv, piece):
    rows, width = q.shape
    nh = width // HD
    keys = kv.shape[0]
    nq = rows // BQ
    row = pl.BlockSpec((BQ, width), lambda i, p: (i, 0))
    gs = pltpu.PrefetchScalarGridSpec(
        num_scalar_prefetch=1, grid=(nq,),
        in_specs=[row, row, row, pl.BlockSpec((1, 8, BQ), lambda i, p: (i, 0, 0)),
                  pl.BlockSpec((keys, 2 * HD), lambda i, p: (0, 0))],
        out_specs=[row, pl.BlockSpec((keys, 2 * HD), lambda i, p: (0, 0))],
        scratch_shapes=[pltpu.VMEM((HD, keys), jnp.bfloat16), pltpu.VMEM((8, BQ), jnp.float32),
                        pltpu.VMEM((width, BQ), jnp.float32)])
    return pl.pallas_call(
        functools.partial(bwd_kernel, nh, piece, keys // piece),
        out_shape=[jax.ShapeDtypeStruct(q.shape, jnp.bfloat16), jax.ShapeDtypeStruct((keys, 2 * HD), jnp.float32)],
        grid_spec=gs, name="attn_bwd", compiler_params=pltpu.CompilerParams(vmem_limit_bytes=VMEM),
        cost_estimate=pl.CostEstimate(flops=150 * 10 ** 9, bytes_accessed=10 ** 7, transcendentals=0))(pos, q, do, o, lse, kv)


def solution(mesh):
    cp_size = mesh.shape['cp']
    row_spec = P(('dp', 'cp', 'tp'), None)

    def local_step(x_blk, dy_blk, w_query, w_key, w_value, w_out):
        rows, d = x_blk.shape
        ng = mesh.shape['tp']
        seq_loc = rows * ng
        piece = seq_loc // 2
        width = w_query.shape[1]
        rank = lax.axis_index('cp')
        half = piece // BQ
        t = jnp.arange(2 * half, dtype=jnp.int32)
        pos = jnp.where(t < half, rank * half + t, (2 * cp_size - 1 - rank) * half + t - half).astype(jnp.int32)

        def a2a(v):
            return lax.all_to_all(v, 'tp', 0, 0, tiled=True)

        wqkv = gather(jnp.concatenate([w_query, w_key, w_value], axis=1), 1, 4)
        q_g, kv_g = qkv_proj(x_blk, wqkv)
        kv_loc = a2a(kv_g).reshape(seq_loc, 2 * HD)
        kv_all = lax.all_gather(kv_loc, 'cp', axis=0, tiled=True)
        q_loc = a2a(q_g).reshape(seq_loc, width)
        w_out, q_g = lax.optimization_barrier((w_out, q_g))
        wo = gather(w_out, 2, 7)
        do_g = do_proj(dy_blk, wo)
        do_loc = a2a(do_g).reshape(seq_loc, width)
        o_loc, lse = attn_fwd(pos, q_loc, kv_all, piece)
        o_g = a2a(o_loc.reshape(ng, rows, width))
        dq_loc, dkv = attn_bwd(pos, q_loc, do_loc, o_loc, lse, kv_all, piece)
        y_blk = y_proj(o_g, wo)
        dq_g = a2a(dq_loc.reshape(ng, rows, width))
        dkv_own = lax.psum_scatter(dkv, 'cp', scatter_dimension=0, tiled=True).astype(jnp.bfloat16)
        dkv_g = a2a(dkv_own.reshape(ng, rows, 2 * HD))
        dx_blk = dx_proj(dq_g, dkv_g, wqkv)
        return y_blk, dx_blk

    return jax.shard_map(local_step, mesh=mesh, in_specs=(row_spec, row_spec, P(None, 'tp'), P(None, 'tp'), P(None, 'tp'), P('tp', None)),
                         out_specs=(row_spec, row_spec), check_vma=False)
```

```python
import functools
import jax
import jax.numpy as jnp
from jax import lax
from jax.experimental import pallas as pl
from jax.experimental.pallas import tpu as pltpu
from jax.sharding import PartitionSpec as P

HD = 128
BQ = 256
LOG2E = 1.4426950408889634
SCALE = HD ** -0.5
NT = (((1,), (1,)), ((), ()))
NN = (((1,), (0,)), ((), ()))
NEG = -1e30
VMEM = 60 * 2 ** 20
MESH_ID = pl.DeviceIdType.MESH


def mm(a, b, dims):
    return lax.dot_general(a, b, dims, preferred_element_type=jnp.float32)


def inphase_kernel(kind, blocks, x_ref, *refs):
    nb = len(blocks)
    n = 3 * nb
    if kind == 'qkv':
        (wq, wk, wv, wall, a_loc, kv_all, wbuf, obuf, res, zs, zr, xs, xr, ys, yr, cs, cr, ls, os, rs, rr,
         kys, kyr, kcs, kcr) = refs
        width = wq.shape[1]
    else:
        (wo, wall, a_loc, wbuf, obuf, res, zs, zr, xs, xr, ys, yr, cs, cr, ls, os, rs, rr) = refs
        width = wo.shape[0]
    x = lax.axis_index('dp')
    z = lax.axis_index('tp')
    cp = lax.axis_index('cp')
    y = cp // 2
    c = cp % 2
    hz = z // 2
    inner = jnp.logical_or(z == 1, z == 2)
    rows = x_ref.shape[0]
    dx = (1 - x, z, cp)
    dy = (x, z, (1 - y) * 2 + c)
    dc = (x, z, y * 2 + 1 - c)
    src = [1 - z + 4 * hz, 2 - hz, 3 - 3 * hz]

    def dz(s):
        return (x, s, cp)

    bar = pltpu.get_barrier_semaphore()
    for d in [dz(src[0]), dz(src[1]), dz(src[2]), dx, dy, dc]:
        pl.semaphore_signal(bar, inc=1, device_id=d, device_id_type=MESH_ID)
    pl.semaphore_wait(bar, 6)

    def eid(xx, yy, cc):
        return (xx * 2 + yy) * 2 + cc

    e0, ex, ey, ed = eid(x, y, c), eid(1 - x, y, c), eid(x, 1 - y, c), eid(1 - x, 1 - y, c)

    def eighth(ref, e, off, size):
        if kind == 'qkv':
            pr = ref.shape[0] // 8
            return ref.at[pl.ds(pl.multiple_of(e * pr, 16), pr), pl.ds(off, size)]
        pr = size // 8
        return ref.at[pl.ds(pl.multiple_of(off + e * pr, 16), pr), :]

    def block(ref, off, size):
        if kind == 'qkv':
            return ref.at[:, pl.ds(off, size)]
        return ref.at[pl.ds(off, size), :]

    def own_parts(j):
        off, size = blocks[j]
        if kind == 'do':
            return [(wo, off, off, size)]
        if off < width:
            return [(wq, off, off, size)]
        return [(wk, 0, width, HD), (wv, 0, width + HD, HD)]

    def rc(a, b, ss, rsem, dev):
        return pltpu.make_async_remote_copy(src_ref=a, dst_ref=b, send_sem=ss, recv_sem=rsem, device_id=dev,
                                            device_id_type=MESH_ID)

    prim, sec = [], []
    for j in range(nb):
        for q, (ref, off, dst, size) in enumerate(own_parts(j)):
            prim.append(rc(eighth(ref, e0, off, size), eighth(wall.at[z], e0, dst, size), zs.at[q, j], zr.at[z, j], dz(src[0])))
            sec.append(rc(eighth(ref, e0, off, size), eighth(wall.at[z], e0, dst, size), zs.at[2 + q, j], zr.at[z, j], dz(3 - z)))
    for q in prim:
        q.start()

    @pl.when(inner)
    def _():
        for q in sec:
            q.start()

    order = [(j, k) for j in range(nb) for k in range(3)]
    zrecv, zfwd, xc, yc, fc, cc = [], [], [], [], [], []
    for i, (j, k) in enumerate(order):
        s = src[k]
        tgt = 3 - z if k == 0 else (z - 1) * 3

        def un(e, s=s, j=j):
            return eighth(wall.at[s], e, *blocks[j])

        zrecv.append(rc(un(e0), un(e0), zs.at[4 + k, j], zr.at[s, j], dz(s)))
        zfwd.append(rc(un(e0), un(e0), zs.at[4 + k, j], zr.at[s, j], dz(tgt)))
        xc.append(rc(un(e0), un(e0), xs.at[i, 0], xr.at[i, 0], dx))
        yc.append(rc(un(e0), un(e0), ys.at[i, 0], yr.at[i, 0], dy))
        if i % 2 == 0:
            fc.append(rc(un(ex), un(ex), ys.at[i, 1], yr.at[i, 1], dy))
        else:
            fc.append(rc(un(ey), un(ey), xs.at[i, 1], xr.at[i, 1], dx))
        cc.append([rc(un(e), un(e), cs.at[i, q], cr.at[i, q], dc) for q, e in enumerate((e0, ex, ey, ed))])

    def st1(i):
        zrecv[i].wait_recv()

        @pl.when(inner)
        def _():
            zfwd[i].start()

        first, second = (xc, yc) if i % 2 == 0 else (yc, xc)
        first[i].start()
        second[i].start()
        cc[i][0].start()

    def st2(i):
        first = xc if i % 2 == 0 else yc
        first[i].wait_recv()
        fc[i].start()
        cc[i][1 if i % 2 == 0 else 2].start()

    def st3(i):
        second = yc if i % 2 == 0 else xc
        second[i].wait_recv()
        cc[i][2 if i % 2 == 0 else 1].start()

    def st4(i):
        fc[i].wait_recv()
        cc[i][3].start()

    def load(i):
        j, k = order[i]
        return pltpu.make_async_copy(block(wall.at[src[k]], *blocks[j]), block(wbuf.at[i % 2], 0, blocks[j][1]), ls.at[i % 2])

    def st5(i):
        for q in cc[i]:
            q.wait_recv()
        load(i).start()

    def project(buf, slot, j):
        off, size = blocks[j]
        if kind == 'qkv':
            r = mm(x_ref[...], buf[:, :size], NN)
        else:
            r = mm(x_ref[...], buf[:size, :], NT)
        res[slot, :, off:off + size] = r.astype(jnp.bfloat16)

    def arow(t):
        return pl.ds(pl.multiple_of(t * rows, 8), rows)

    def kvrow(p, t):
        return kv_all.at[pl.ds(pl.multiple_of((p * 4 + t) * rows, 8), rows), :]

    def result(slot, j, t):
        off, size = blocks[j]
        here = res.at[slot, :, pl.ds(off, size)]
        if off >= width:
            return here, kvrow(cp, t)
        return here, a_loc.at[arow(t), pl.ds(off, size)]

    rsend = {(j, k): rc(*result(k, j, z), rs.at[j, k], rr.at[z, j], dz(src[k])) for j, k in order}
    rrecv = {(j, k): rc(*result(k, j, src[k]), rs.at[j, k], rr.at[src[k], j], dz(src[k])) for j, k in order}

    def st6(i):
        j, k = order[i]
        load(i).wait()
        project(wbuf.at[i % 2], k, j)
        rsend[j, k].start()

    def own_in(j):
        return [pltpu.make_async_copy(block(ref, off, size), block(obuf.at[j % 2], dst - blocks[j][0], size), os.at[j % 2, q])
                for q, (ref, off, dst, size) in enumerate(own_parts(j))]

    def own_out(j):
        return pltpu.make_async_copy(block(obuf.at[j % 2], 0, blocks[j][1]), block(wall.at[z], *blocks[j]), os.at[j % 2, 2])

    def own_res(j):
        return pltpu.make_async_copy(*result(3, j, z), os.at[2 + j, 0])

    def own_start(j):
        if j >= 2:
            own_out(j - 2).wait()
        for q in own_in(j):
            q.start()

    def own_do(j):
        for q in own_in(j):
            q.wait()
        own_out(j).start()
        project(obuf.at[j % 2], 3, j)
        own_res(j).start()

    if kind == 'qkv':
        py = (1 - y) * 2 + c
        ts = [z] + src
        kyc = [rc(kvrow(cp, t), kvrow(cp, t), kys.at[j], kyr.at[j], dy) for j, t in enumerate(ts)]
        kyr_ = [rc(kvrow(py, t), kvrow(py, t), kys.at[j], kyr.at[j], dy) for j, t in enumerate(ts)]
        kcc = [rc(kvrow(cp, t), kvrow(cp, t), kcs.at[j, 0], kcr.at[j, 0], dc) for j, t in enumerate(ts)]
        kcf = [rc(kvrow(py, t), kvrow(py, t), kcs.at[j, 1], kcr.at[j, 1], dc) for j, t in enumerate(ts)]

        def kv1(j):
            if j == 0:
                own_res(0).wait()
            else:
                rrecv[0, j - 1].wait_recv()
            kyc[j].start()
            kcc[j].start()

        def kv2(j):
            kyr_[j].wait_recv()
            kcf[j].start()

    own_start(0)
    own_start(1)
    later = {}

    def at(i, f, *args):
        later.setdefault(i, []).append(functools.partial(f, *args))

    for j in range(nb):
        at(3 * j + 1, own_do, j)
        if j + 2 < nb:
            at(3 * j + 2, own_start, j + 2)
    if kind == 'qkv':
        at(3, kv1, 0)
        for j in range(1, 4):
            at(7 + j, kv1, j)
        for j in range(4):
            at(9 + j, kv2, j)
    for i in range(max(n + 6, max(later) + 1)):
        if i < n:
            st1(i)
        if 0 <= i - 1 < n:
            st2(i - 1)
        if 0 <= i - 2 < n:
            st3(i - 2)
        if 0 <= i - 3 < n:
            st4(i - 3)
        if 0 <= i - 5 < n:
            st6(i - 5)
        if 0 <= i - 4 < n:
            st5(i - 4)
        for f in later.get(i, []):
            f()

    for q in prim:
        q.wait_send()

    @pl.when(inner)
    def _():
        for q in sec + zfwd:
            q.wait_send()

    for i in range(n):
        for q in [xc[i], yc[i], fc[i]] + cc[i]:
            q.wait_send()
    for j in range(nb):
        if j >= nb - 2:
            own_out(j).wait()
        if not (kind == 'qkv' and j == 0):
            own_res(j).wait()
        for k in range(3):
            rsend[j, k].wait_send()
            if not (kind == 'qkv' and j == 0):
                rrecv[j, k].wait_recv()
    if kind == 'qkv':
        for j in range(4):
            kyc[j].wait_send()
            kcc[j].wait_send()
            kcf[j].wait_send()
            kcc[j].wait_recv()
            kcf[j].wait_recv()


def inphase(kind, x, ws, blocks, cid):
    rows, d = x.shape
    qkv = kind == 'qkv'
    cols = sum(w.shape[1] for w in ws) if qkv else ws[0].shape[0]
    width = cols - 2 * HD if qkv else cols
    big = max(b[1] for b in blocks)
    dma = pltpu.SemaphoreType.DMA
    nb = len(blocks)
    n = 3 * nb
    hbm = pl.BlockSpec(memory_space=pltpu.HBM)
    bf = jnp.bfloat16
    out_shape = [jax.ShapeDtypeStruct((4, d, cols) if qkv else (4, cols, d), bf), jax.ShapeDtypeStruct((4 * rows, width), bf)]
    tile = (2, d, big) if qkv else (2, big, d)
    scratch = [pltpu.VMEM(tile, bf), pltpu.VMEM(tile, bf), pltpu.VMEM((4, rows, cols), bf),
               dma((7, nb)), dma((4, nb)), dma((n, 2)), dma((n, 2)), dma((n, 2)), dma((n, 2)), dma((n, 4)), dma((n, 4)),
               dma((2,)), dma((2 + nb, 3)), dma((nb, 3)), dma((4, nb))]
    if qkv:
        out_shape.append(jax.ShapeDtypeStruct((16 * rows, 2 * HD), bf))
        scratch += [dma((4,)), dma((4,)), dma((4, 2)), dma((4, 2))]
    return pl.pallas_call(
        functools.partial(inphase_kernel, kind, blocks),
        out_shape=out_shape,
        in_specs=[pl.BlockSpec(memory_space=pltpu.VMEM)] + [hbm] * len(ws),
        out_specs=[hbm] * len(out_shape),
        scratch_shapes=scratch,
        name=f"inphase_{kind}",
        compiler_params=pltpu.CompilerParams(collective_id=cid, has_side_effects=True, vmem_limit_bytes=VMEM),
        cost_estimate=pl.CostEstimate(flops=10 ** 11, bytes_accessed=10 ** 7, transcendentals=0))(x, *ws)


def split_blocks(total, size):
    return [(o, min(size, total - o)) for o in range(0, total, size)]


def y_kernel(o_ref, w_ref, y_ref):
    acc = mm(o_ref[0], w_ref[0], NN)
    for g in range(1, o_ref.shape[0]):
        acc = acc + mm(o_ref[g], w_ref[g], NN)
    y_ref[...] = acc.astype(jnp.bfloat16)


def y_proj(o, wo):
    ng, rows, nq = o.shape
    d = wo.shape[2]
    bn = 512
    return pl.pallas_call(
        y_kernel, grid=(d // bn,),
        out_shape=jax.ShapeDtypeStruct((rows, d), jnp.bfloat16),
        in_specs=[pl.BlockSpec((ng, rows, nq), lambda j: (0, 0, 0)), pl.BlockSpec((ng, nq, bn), lambda j: (0, 0, j))],
        out_specs=pl.BlockSpec((rows, bn), lambda j: (0, j)),
        name="y_proj", compiler_params=pltpu.CompilerParams(vmem_limit_bytes=VMEM),
        cost_estimate=pl.CostEstimate(flops=2 * rows * d * nq * ng, bytes_accessed=30 * 10 ** 6, transcendentals=0))(o, wo)


def dx_kernel(dq_ref, dkv_ref, w_ref, dx_ref):
    nq = dq_ref.shape[2]
    acc = None
    for g in range(dq_ref.shape[0]):
        t = mm(dq_ref[g], w_ref[g, :, :nq], NT) + mm(dkv_ref[g], w_ref[g, :, nq:], NT)
        acc = t if acc is None else acc + t
    dx_ref[...] = acc.astype(jnp.bfloat16)


def dx_proj(dq, dkv, wqkv):
    ng, rows, nq = dq.shape
    _, d, cols = wqkv.shape
    bn = 512
    return pl.pallas_call(
        dx_kernel, grid=(d // bn,),
        out_shape=jax.ShapeDtypeStruct((rows, d), jnp.bfloat16),
        in_specs=[pl.BlockSpec((ng, rows, nq), lambda j: (0, 0, 0)), pl.BlockSpec((ng, rows, 2 * HD), lambda j: (0, 0, 0)),
                  pl.BlockSpec((ng, bn, cols), lambda j: (0, j, 0))],
        out_specs=pl.BlockSpec((rows, bn), lambda j: (0, j)),
        name="dx_proj", compiler_params=pltpu.CompilerParams(vmem_limit_bytes=VMEM),
        cost_estimate=pl.CostEstimate(flops=2 * rows * d * cols * ng, bytes_accessed=40 * 10 ** 6, transcendentals=0))(dq, dkv, wqkv)


def piece_row(j, piece, n_pieces):
    half = n_pieces // 2
    return jnp.where(j < half, j * 2 * piece, (n_pieces - 1 - j) * 2 * piece + piece)


def key_loop(n, piece, n_pieces, tile):
    per = piece // BQ
    full = n // per

    def whole(j, _):
        tile(pl.multiple_of(piece_row(j, piece, n_pieces), BQ), piece, False)
        return 0

    def part(j, _):
        tile(pl.multiple_of(piece_row(full, piece, n_pieces) + (j - full * per) * BQ, BQ), BQ, False)
        return 0

    lax.fori_loop(0, full, whole, 0)
    lax.fori_loop(full * per, n, part, 0)
    tile(pl.multiple_of(piece_row(full, piece, n_pieces) + (n - full * per) * BQ, BQ), BQ, True)


def keep_mask(size):
    r = lax.broadcasted_iota(jnp.int32, (size, BQ), 0)
    q = lax.broadcasted_iota(jnp.int32, (size, BQ), 1)
    return r <= q


def fwd_kernel(nh, piece, n_pieces, pos_ref, q_ref, kv_ref, o_ref, lse_ref, vt_ref, m_ref, l_ref, acc_ref):
    i = pl.program_id(0)
    n = pos_ref[i]

    @pl.when(i == 0)
    def _():
        for b in range(n_pieces):
            vt_ref[:, b * piece:(b + 1) * piece] = kv_ref[b * piece:(b + 1) * piece, HD:].T

    m_ref[...] = jnp.full_like(m_ref, NEG)
    l_ref[...] = jnp.zeros_like(l_ref)
    acc_ref[...] = jnp.zeros_like(acc_ref)

    def tile(start, size, masked):
        k = kv_ref[pl.ds(start, size), :HD]
        vt = vt_ref[:, pl.ds(start, size)]
        scores = [mm(k, q_ref[:, h * HD:(h + 1) * HD], NT) for h in range(nh)]
        for h in range(nh):
            s = scores[h] * (SCALE * LOG2E)
            if masked:
                s = jnp.where(keep_mask(size), s, NEG)
            m_old = m_ref[h:h + 1, :]
            m_new = jnp.maximum(m_old, jnp.max(s, axis=0, keepdims=True))
            p = jnp.exp2(s - m_new)
            a = jnp.exp2(m_old - m_new)
            m_ref[h:h + 1, :] = m_new
            l_ref[h:h + 1, :] = l_ref[h:h + 1, :] * a + jnp.sum(p, axis=0, keepdims=True)
            o = mm(vt, p.astype(jnp.bfloat16), NN)
            acc_ref[h * HD:(h + 1) * HD, :] = acc_ref[h * HD:(h + 1) * HD, :] * a + o

    key_loop(n, piece, n_pieces, tile)
    for h in range(nh):
        l = l_ref[h:h + 1, :]
        o = acc_ref[h * HD:(h + 1) * HD, :] / l
        o_ref[:, h * HD:(h + 1) * HD] = o.T.astype(jnp.bfloat16)
        lse_ref[0, h:h + 1, :] = m_ref[h:h + 1, :] + jnp.log2(l)


def attn_fwd(pos, q, kv, piece):
    rows, width = q.shape
    nh = width // HD
    keys = kv.shape[0]
    nq = rows // BQ
    gs = pltpu.PrefetchScalarGridSpec(
        num_scalar_prefetch=1, grid=(nq,),
        in_specs=[pl.BlockSpec((BQ, width), lambda i, p: (i, 0)), pl.BlockSpec((keys, 2 * HD), lambda i, p: (0, 0))],
        out_specs=[pl.BlockSpec((BQ, width), lambda i, p: (i, 0)), pl.BlockSpec((1, 8, BQ), lambda i, p: (i, 0, 0))],
        scratch_shapes=[pltpu.VMEM((HD, keys), jnp.bfloat16), pltpu.VMEM((8, BQ), jnp.float32),
                        pltpu.VMEM((8, BQ), jnp.float32), pltpu.VMEM((width, BQ), jnp.float32)])
    return pl.pallas_call(
        functools.partial(fwd_kernel, nh, piece, keys // piece),
        out_shape=[jax.ShapeDtypeStruct(q.shape, jnp.bfloat16), jax.ShapeDtypeStruct((nq, 8, BQ), jnp.float32)],
        grid_spec=gs, name="attn_fwd", compiler_params=pltpu.CompilerParams(vmem_limit_bytes=VMEM),
        cost_estimate=pl.CostEstimate(flops=64 * 10 ** 9, bytes_accessed=10 ** 7, transcendentals=0))(pos, q, kv)


def bwd_kernel(nh, piece, n_pieces, pos_ref, q_ref, do_ref, o_ref, lse_ref, kv_ref, dq_ref, dkv_ref, kt_ref, del_ref, dqt_ref):
    i = pl.program_id(0)
    n = pos_ref[i]

    @pl.when(i == 0)
    def _():
        dkv_ref[...] = jnp.zeros_like(dkv_ref)
        for b in range(n_pieces):
            kt_ref[:, b * piece:(b + 1) * piece] = kv_ref[b * piece:(b + 1) * piece, :HD].T

    for h in range(nh):
        sl = slice(h * HD, (h + 1) * HD)
        pr = do_ref[:, sl].astype(jnp.float32) * o_ref[:, sl].astype(jnp.float32)
        del_ref[h:h + 1, :] = jnp.sum(pr.T, axis=0, keepdims=True)
    dqt_ref[...] = jnp.zeros_like(dqt_ref)

    def tile(start, size, masked):
        for t0 in range(0, size, BQ):
            sub(start + t0, masked)

    def sub(start, masked):
        size = BQ
        k = kv_ref[pl.ds(start, size), :HD]
        v = kv_ref[pl.ds(start, size), HD:]
        kt = kt_ref[:, pl.ds(start, size)]
        dv = None
        dk = None
        for h in range(nh):
            sl = slice(h * HD, (h + 1) * HD)
            s = mm(k, q_ref[:, sl], NT) * (SCALE * LOG2E) - lse_ref[0, h:h + 1, :]
            dp = mm(v, do_ref[:, sl], NT)
            if masked:
                s = jnp.where(keep_mask(size), s, NEG)
            pb = jnp.exp2(s).astype(jnp.bfloat16)
            ds = (pb.astype(jnp.float32) * (dp - del_ref[h:h + 1, :])).astype(jnp.bfloat16)
            dvh = mm(pb, do_ref[:, sl], NN)
            dkh = mm(ds, q_ref[:, sl], NN)
            dv = dvh if dv is None else dv + dvh
            dk = dkh if dk is None else dk + dkh
            dqt_ref[sl, :] += mm(kt, ds, NN)
        dkv_ref[pl.ds(start, size), :HD] += dk * SCALE
        dkv_ref[pl.ds(start, size), HD:] += dv

    key_loop(n, piece, n_pieces, tile)
    for h in range(nh):
        sl = slice(h * HD, (h + 1) * HD)
        dq_ref[:, sl] = (dqt_ref[sl, :] * SCALE).T.astype(jnp.bfloat16)


def attn_bwd(pos, q, do, o, lse, kv, piece):
    rows, width = q.shape
    nh = width // HD
    keys = kv.shape[0]
    nq = rows // BQ
    row = pl.BlockSpec((BQ, width), lambda i, p: (i, 0))
    gs = pltpu.PrefetchScalarGridSpec(
        num_scalar_prefetch=1, grid=(nq,),
        in_specs=[row, row, row, pl.BlockSpec((1, 8, BQ), lambda i, p: (i, 0, 0)),
                  pl.BlockSpec((keys, 2 * HD), lambda i, p: (0, 0))],
        out_specs=[row, pl.BlockSpec((keys, 2 * HD), lambda i, p: (0, 0))],
        scratch_shapes=[pltpu.VMEM((HD, keys), jnp.bfloat16), pltpu.VMEM((8, BQ), jnp.float32),
                        pltpu.VMEM((width, BQ), jnp.float32)])
    return pl.pallas_call(
        functools.partial(bwd_kernel, nh, piece, keys // piece),
        out_shape=[jax.ShapeDtypeStruct(q.shape, jnp.bfloat16), jax.ShapeDtypeStruct((keys, 2 * HD), jnp.float32)],
        grid_spec=gs, name="attn_bwd", compiler_params=pltpu.CompilerParams(vmem_limit_bytes=VMEM),
        cost_estimate=pl.CostEstimate(flops=150 * 10 ** 9, bytes_accessed=10 ** 7, transcendentals=0))(pos, q, do, o, lse, kv)


def solution(mesh):
    cp_size = mesh.shape['cp']
    row_spec = P(('dp', 'cp', 'tp'), None)

    def local_step(x_blk, dy_blk, w_query, w_key, w_value, w_out):
        rows, d = x_blk.shape
        ng = mesh.shape['tp']
        seq_loc = rows * ng
        piece = seq_loc // 2
        width = w_query.shape[1]
        rank = lax.axis_index('cp')
        half = piece // BQ
        t = jnp.arange(2 * half, dtype=jnp.int32)
        pos = jnp.where(t < half, rank * half + t, (2 * cp_size - 1 - rank) * half + t - half).astype(jnp.int32)

        def a2a(v):
            return lax.all_to_all(v, 'tp', 0, 0, tiled=True)

        qkv_blocks = [(width, 2 * HD)] + split_blocks(width, 256)
        wqkv, q_loc, kv_all = inphase('qkv', x_blk, [w_query, w_key, w_value], qkv_blocks, 1)
        w_out, q_loc = lax.optimization_barrier((w_out, q_loc))
        wo, do_loc = inphase('do', dy_blk, [w_out], split_blocks(width, 256), 2)
        o_loc, lse = attn_fwd(pos, q_loc, kv_all, piece)
        o_g = a2a(o_loc.reshape(ng, rows, width))
        dq_loc, dkv = attn_bwd(pos, q_loc, do_loc, o_loc, lse, kv_all, piece)
        y_blk = y_proj(o_g, wo)
        dq_g = a2a(dq_loc.reshape(ng, rows, width))
        dkv_own = lax.psum_scatter(dkv, 'cp', scatter_dimension=0, tiled=True).astype(jnp.bfloat16)
        dkv_g = a2a(dkv_own.reshape(ng, rows, 2 * HD))
        dx_blk = dx_proj(dq_g, dkv_g, wqkv)
        return y_blk, dx_blk

    return jax.shard_map(local_step, mesh=mesh, in_specs=(row_spec, row_spec, P(None, 'tp'), P(None, 'tp'), P(None, 'tp'), P('tp', None)),
                         out_specs=(row_spec, row_spec), check_vma=False)
```

```python
import functools
import jax
import jax.numpy as jnp
from jax import lax
from jax.experimental import pallas as pl
from jax.experimental.pallas import tpu as pltpu
from jax.sharding import PartitionSpec as P

HD = 128
BQ = 256
LOG2E = 1.4426950408889634
SCALE = HD ** -0.5
NT = (((1,), (1,)), ((), ()))
NN = (((1,), (0,)), ((), ()))
NEG = -1e30
VMEM = 60 * 2 ** 20
MESH_ID = pl.DeviceIdType.MESH


def mm(a, b, dims):
    return lax.dot_general(a, b, dims, preferred_element_type=jnp.float32)


def input_kernel(piece, n_pieces, x_ref, dy_ref, wq, wk, wv, wo, wqkv_all, wo_all, q_loc, kv_all, do_loc, o_loc, lse_ref,
                 wbuf, vbuf, obuf, pbuf, res, resd, qv, kvv, vt_ref, m_ref, l_ref, acc_ref, ost,
                 zs, zr, xs, xr, ys, yr, cs, cr, ls, os, orr, rs, rr, kys, kyr, kcs, kcr, fs):
    width = wq.shape[1]
    nh = width // HD
    nkv = nh + 2
    nb = nkv + nh
    n = 3 * nb
    x = lax.axis_index('dp')
    z = lax.axis_index('tp')
    cp = lax.axis_index('cp')
    y = cp // 2
    c = cp % 2
    hz = z // 2
    inner = jnp.logical_or(z == 1, z == 2)
    rows = x_ref.shape[0]
    dx = (1 - x, z, cp)
    dy = (x, z, (1 - y) * 2 + c)
    dc = (x, z, y * 2 + 1 - c)
    src = [1 - z + 4 * hz, 2 - hz, 3 - 3 * hz]

    def dz(s):
        return (x, s, cp)

    bar = pltpu.get_barrier_semaphore()
    for d in [dz(src[0]), dz(src[1]), dz(src[2]), dx, dy, dc]:
        pl.semaphore_signal(bar, inc=1, device_id=d, device_id_type=MESH_ID)
    pl.semaphore_wait(bar, 6)

    def eid(xx, yy, cc):
        return (xx * 2 + yy) * 2 + cc

    e0, ex, ey, ed = eid(x, y, c), eid(1 - x, y, c), eid(x, 1 - y, c), eid(1 - x, 1 - y, c)
    dk = wq.shape[0] // 8
    dr = HD // 8

    def by_kind(j, f):
        def qkv():
            f(True, pl.multiple_of(jnp.where(j < 2, width + j * HD, (j - 2) * HD), HD))

        def out():
            f(False, pl.multiple_of((j - nkv) * HD, HD))

        if isinstance(j, int):
            qkv() if j < nkv else out()
        else:
            pl.when(j < nkv)(qkv)
            pl.when(j >= nkv)(out)

    def block(qkv, s, off):
        return wqkv_all.at[s, :, pl.ds(off, HD)] if qkv else wo_all.at[s, pl.ds(off, HD), :]

    def eighth(qkv, s, e, off):
        if qkv:
            return wqkv_all.at[s, pl.ds(pl.multiple_of(e * dk, 16), dk), pl.ds(off, HD)]
        return wo_all.at[s, pl.ds(pl.multiple_of(off + e * dr, 16), dr), :]

    def own_block(j):
        if j < 2:
            return (wk, wv)[j], 0
        return (wq, (j - 2) * HD) if j < nkv else (wo, (j - nkv) * HD)

    def rc(a, b, ss, rsem, dev):
        return pltpu.make_async_remote_copy(src_ref=a, dst_ref=b, send_sem=ss, recv_sem=rsem, device_id=dev,
                                            device_id_type=MESH_ID)

    def own_piece(j):
        ref, off = own_block(j)
        if j < nkv:
            return ref.at[pl.ds(pl.multiple_of(e0 * dk, 16), dk), pl.ds(off, HD)]
        return ref.at[pl.ds(pl.multiple_of(off + e0 * dr, 16), dr), :]

    prim, sec = [], []
    for j in range(nb):
        dst = []
        by_kind(j, lambda qkv, off: dst.append(eighth(qkv, z, e0, off)))
        prim.append(rc(own_piece(j), dst[0], zs.at[0, j], zr.at[z, j], dz(src[0])))
        sec.append(rc(own_piece(j), dst[0], zs.at[1, j], zr.at[z, j], dz(3 - z)))

    def own_send(j0, j1):
        for q in prim[j0:j1]:
            q.start()

        @pl.when(inner)
        def _():
            for q in sec[j0:j1]:
                q.start()

    own_send(0, nkv)

    def unit(i):
        j, k = i // 3, i % 3
        return j, k, jnp.where(k == 0, src[0], jnp.where(k == 1, src[1], src[2]))

    def copies(i, qkv, off):
        j, k, s = unit(i)
        tgt = jnp.where(k == 0, 3 - z, (z - 1) * 3)
        un = functools.partial(eighth, qkv, s, off=off)
        d = dict(zr=rc(un(e0), un(e0), zs.at[2 + k, j], zr.at[s, j], dz(s)),
                 zf=rc(un(e0), un(e0), zs.at[2 + k, j], zr.at[s, j], dz(tgt)),
                 x=rc(un(e0), un(e0), xs.at[i, 0], xr.at[i, 0], dx),
                 y=rc(un(e0), un(e0), ys.at[i, 0], yr.at[i, 0], dy),
                 fy=rc(un(ex), un(ex), ys.at[i, 1], yr.at[i, 1], dy),
                 fx=rc(un(ey), un(ey), xs.at[i, 1], xr.at[i, 1], dx))
        for q, e in enumerate((e0, ex, ey, ed)):
            d[q] = rc(un(e), un(e), cs.at[i, q], cr.at[i, q], dc)
        return d

    def stage(i, f):
        def run(qkv, off):
            d = copies(i, qkv, off)
            pl.when(i % 2 == 0)(functools.partial(f, d, True))
            pl.when(i % 2 == 1)(functools.partial(f, d, False))

        @pl.when(jnp.logical_and(i >= 0, i < n))
        def _():
            by_kind(i // 3, run)

    def st1(d, even):
        d['zr'].wait_recv()

        @pl.when(inner)
        def _():
            d['zf'].start()

        d['x' if even else 'y'].start()
        d['y' if even else 'x'].start()
        d[0].start()

    def st2(d, even):
        d['x' if even else 'y'].wait_recv()
        d['fy' if even else 'fx'].start()
        d[1 if even else 2].start()

    def st3(d, even):
        d['y' if even else 'x'].wait_recv()
        d[2 if even else 1].start()

    def st4(d, even):
        d['fy' if even else 'fx'].wait_recv()
        d[3].start()

    def arow(t):
        return pl.ds(pl.multiple_of(t * rows, 16), rows)

    def kvrow(p, t):
        return pl.ds(pl.multiple_of((p * 4 + t) * rows, 16), rows)

    def project(qkv, buf, slot, off):
        step = rows // 3

        def part(r, _):
            w = pl.ds(pl.multiple_of(r * step, 16), step)
            if qkv:
                res[slot, w, pl.ds(off, HD)] = mm(x_ref[w, :], buf, NN).astype(jnp.bfloat16)
            else:
                resd[slot, w, pl.ds(off, HD)] = mm(dy_ref[w, :], buf, NT).astype(jnp.bfloat16)
            return 0

        lax.fori_loop(0, 3, part, 0)

    def result(j, slot, t, f):
        def run(qkv, off):
            here = (res if qkv else resd).at[slot, :, pl.ds(off, HD)]
            if not qkv:
                f(here, do_loc.at[arow(t), pl.ds(off, HD)])
                return

            @pl.when(j < 2)
            def _():
                f(here, kv_all.at[kvrow(cp, t), pl.ds(pl.multiple_of(j * HD, HD), HD)])

            @pl.when(j >= 2)
            def _():
                f(here, q_loc.at[arow(t), pl.ds(off, HD)])

        by_kind(j, run)

    def load(i, qkv, off):
        _, _, s = unit(i)
        return pltpu.make_async_copy(block(qkv, s, off), (wbuf if qkv else vbuf).at[i % 2], ls.at[i % 2])

    def st5(i):
        @pl.when(jnp.logical_and(i >= 0, i < n))
        def _():
            def run(qkv, off):
                d = copies(i, qkv, off)
                for q in range(4):
                    d[q].wait_recv()
                load(i, qkv, off).start()

            by_kind(i // 3, run)

    def st6(i):
        @pl.when(jnp.logical_and(i >= 0, i < n))
        def _():
            j, k, s = unit(i)

            def run(qkv, off):
                load(i, qkv, off).wait()
                project(qkv, (wbuf if qkv else vbuf)[i % 2], k, off)

            by_kind(j, run)
            result(j, k, z, lambda a, b: rc(a, b, rs.at[j, k], rr.at[z, j], dz(s)).start())

    def own_in(j, f):
        def run(qkv, off):
            buf = (obuf if qkv else pbuf).at[j % 2]
            if not qkv:
                f(pltpu.make_async_copy(wo.at[pl.ds(off, HD), :], buf, os.at[j % 2]))
            elif isinstance(j, int) and j < 2:
                f(pltpu.make_async_copy((wk, wv)[j], buf, os.at[j % 2]))
            else:
                f(pltpu.make_async_copy(wq.at[:, pl.ds(off, HD)], buf, os.at[j % 2]))

        by_kind(j, run)

    def own_do(j):
        own_in(j, lambda q: q.wait())

        def run(qkv, off):
            buf = (obuf if qkv else pbuf)
            keep = pltpu.make_async_copy(buf.at[j % 2], block(qkv, z, off), os.at[2])
            keep.start()
            project(qkv, buf[j % 2], 3, off)
            keep.wait()

        by_kind(j, run)
        result(j, 3, z, lambda a, b: pltpu.make_async_copy(a, b, orr.at[j]).start())

    def own_wait(j0, j1):
        for j in range(j0, j1):
            if j < 2:
                pltpu.make_async_copy(res.at[3, :, pl.ds(width + j * HD, HD)], kv_all.at[kvrow(cp, z), pl.ds(j * HD, HD)], orr.at[j]).wait()
            elif j < nkv:
                pltpu.make_async_copy(res.at[3, :, pl.ds((j - 2) * HD, HD)], q_loc.at[arow(z), pl.ds((j - 2) * HD, HD)], orr.at[j]).wait()
            else:
                o = (j - nkv) * HD
                pltpu.make_async_copy(resd.at[3, :, pl.ds(o, HD)], do_loc.at[arow(z), pl.ds(o, HD)], orr.at[j]).wait()

    def got(j0, j1):
        for j in range(j0, j1):
            for k in range(3):
                t = src[k]
                if j < 2:
                    a = kv_all.at[kvrow(cp, t), pl.ds(j * HD, HD)]
                elif j < nkv:
                    a = q_loc.at[arow(t), pl.ds((j - 2) * HD, HD)]
                else:
                    a = do_loc.at[arow(t), pl.ds((j - nkv) * HD, HD)]
                rc(a, a, rs.at[j, k], rr.at[t, j], dz(t)).wait_recv()

    py = (1 - y) * 2 + c
    ts = [z] + src
    kva = [kv_all.at[kvrow(cp, t), :] for t in ts]
    kvb = [kv_all.at[kvrow(py, t), :] for t in ts]
    kyc = [rc(a, a, kys.at[j], kyr.at[j], dy) for j, a in enumerate(kva)]
    kyg = [rc(a, a, kys.at[j], kyr.at[j], dy) for j, a in enumerate(kvb)]
    kcc = [rc(a, a, kcs.at[j, 0], kcr.at[j, 0], dc) for j, a in enumerate(kva)]
    kcf = [rc(a, a, kcs.at[j, 1], kcr.at[j, 1], dc) for j, a in enumerate(kvb)]

    def kv1(j):
        if j == 0:
            own_wait(0, 2)
        else:
            t = ts[j]
            for b in range(2):
                a = kv_all.at[kvrow(cp, t), pl.ds(b * HD, HD)]
                rc(a, a, rs.at[b, j - 1], rr.at[t, b], dz(t)).wait_recv()
        kyc[j].start()
        kcc[j].start()

    def kv2(j):
        kyg[j].wait_recv()
        kcf[j].start()

    per = piece // BQ
    n_units = per * (n_pieces + 1)
    load_q = pltpu.make_async_copy(q_loc, qv, fs.at[0])
    load_kv = pltpu.make_async_copy(kv_all, kvv, fs.at[1])

    def fwd_load():
        for j in range(4):
            kcc[j].wait_recv()
            kcf[j].wait_recv()
        load_kv.start()
        own_wait(2, nkv)
        got(2, nkv)
        load_q.start()
        load_kv.wait()
        for b in range(n_pieces):
            vt_ref[:, b * piece:(b + 1) * piece] = kvv[b * piece:(b + 1) * piece, HD:].T
        load_q.wait()

    def o_out(i):
        return pltpu.make_async_copy(ost.at[i % 2], o_loc.at[pl.ds(pl.multiple_of(i * BQ, BQ), BQ), :], fs.at[2 + i % 2])

    def fwd_unit(u):
        n0 = cp + 1
        n1 = n_pieces - cp
        early = u < per * n0
        v = u - per * n0
        i = jnp.where(early, u // n0, per + v // n1)
        j = jnp.where(early, u % n0, v % n1)
        diag = j == jnp.where(early, n0, n1) - 1
        start = pl.multiple_of(piece_row(j, piece, n_pieces), BQ)
        qrow = pl.ds(pl.multiple_of(i * BQ, BQ), BQ)

        @pl.when(j == 0)
        def _():
            m_ref[...] = jnp.full_like(m_ref, NEG)
            l_ref[...] = jnp.zeros_like(l_ref)
            acc_ref[...] = jnp.zeros_like(acc_ref)

        def tile(masked):
            k = kvv[pl.ds(start, piece), :HD]
            vt = vt_ref[:, pl.ds(start, piece)]
            if masked:
                kr = lax.broadcasted_iota(jnp.int32, (piece, BQ), 0)
                qr = lax.broadcasted_iota(jnp.int32, (piece, BQ), 1)
                keep = kr <= qr + (i % per) * BQ
            scores = [mm(k, qv[qrow, h * HD:(h + 1) * HD], NT) for h in range(nh)]
            for h in range(nh):
                s = scores[h] * (SCALE * LOG2E)
                if masked:
                    s = jnp.where(keep, s, NEG)
                m_old = m_ref[h:h + 1, :]
                m_new = jnp.maximum(m_old, jnp.max(s, axis=0, keepdims=True))
                p = jnp.exp2(s - m_new)
                a = jnp.exp2(m_old - m_new)
                m_ref[h:h + 1, :] = m_new
                l_ref[h:h + 1, :] = l_ref[h:h + 1, :] * a + jnp.sum(p, axis=0, keepdims=True)
                o = mm(vt, p.astype(jnp.bfloat16), NN)
                acc_ref[h * HD:(h + 1) * HD, :] = acc_ref[h * HD:(h + 1) * HD, :] * a + o

        @pl.when(jnp.logical_not(diag))
        def _():
            tile(False)

        @pl.when(diag)
        def _():
            tile(True)

            @pl.when(i >= 2)
            def _():
                o_out(i).wait()

            for h in range(nh):
                l = l_ref[h:h + 1, :]
                o = acc_ref[h * HD:(h + 1) * HD, :] / l
                ost[i % 2, :, h * HD:(h + 1) * HD] = o.T.astype(jnp.bfloat16)
                lse_ref[i, h:h + 1, :] = m_ref[h:h + 1, :] + jnp.log2(l)
            o_out(i).start()

    own_in(0, lambda q: q.start())
    own_in(1, lambda q: q.start())
    own_do(0)
    own_in(2, lambda q: q.start())
    own_do(1)

    f0 = 3 * nkv + FWD_AT
    f1 = n + 5

    def once(i, at, f, *args):
        pl.when(i == at)(functools.partial(f, *args))

    def step(i, _):
        stage(i, st1)
        stage(i - 1, st2)
        stage(i - 2, st3)
        stage(i - 3, st4)
        st6(i - 5)
        st5(i - 4)
        j = i // 3

        @pl.when(jnp.logical_and(i % 3 == 1, jnp.logical_and(j >= 2, j < nb)))
        def _():
            own_do(j)

        @pl.when(jnp.logical_and(i % 3 == 2, jnp.logical_and(j >= 2, j + 1 < nb)))
        def _():
            own_in(j + 1, lambda q: q.start())

        once(i, 2, kv1, 0)
        for k in range(1, 4):
            once(i, 9 + k, kv1, k)
        for k in range(4):
            once(i, 12 + k, kv2, k)
        once(i, 2 * nkv, own_send, nkv, nb)
        once(i, f0, fwd_load)

        @pl.when(i > f0)
        def _():
            lax.fori_loop(n_units * (i - 1 - f0) // (f1 - f0), n_units * (i - f0) // (f1 - f0), lambda u, _: (fwd_unit(u), 0)[1], 0)

        return 0

    lax.fori_loop(0, f1 + 1, step, 0)

    for i in range(2 * per - 2, 2 * per):
        o_out(i).wait()
    for q in prim:
        q.wait_send()

    @pl.when(inner)
    def _():
        for q in sec:
            q.wait_send()

    def drain(i, _):
        def f(d, even):
            @pl.when(inner)
            def _():
                d['zf'].wait_send()
            for q in ['x', 'y', 'fy' if even else 'fx', 0, 1, 2, 3]:
                d[q].wait_send()

        stage(i, f)
        j, k, s = unit(i)
        result(j, k, z, lambda a, b: rc(a, b, rs.at[j, k], rr.at[z, j], dz(s)).wait_send())
        return 0

    lax.fori_loop(0, n, drain, 0)
    own_wait(nkv, nb)
    got(nkv, nb)
    for j in range(4):
        kyc[j].wait_send()
        kcc[j].wait_send()
        kcf[j].wait_send()


FWD_AT = 9


def input_phase(x, dy, wq, wk, wv, wo, cp_size):
    rows, d = x.shape
    width = wq.shape[1]
    cols = width + 2 * HD
    nb = 2 * (width // HD) + 2
    n = 3 * nb
    seq = 4 * rows
    piece = seq // 2
    keys = seq * cp_size
    bf, f32 = jnp.bfloat16, jnp.float32
    dma = pltpu.SemaphoreType.DMA
    hbm = pl.BlockSpec(memory_space=pltpu.HBM)
    vmem = pl.BlockSpec(memory_space=pltpu.VMEM)
    sds = jax.ShapeDtypeStruct
    out_shape = [sds((4, d, cols), bf), sds((4, width, d), bf), sds((seq, width), bf), sds((keys, 2 * HD), bf),
                 sds((seq, width), bf), sds((seq, width), bf), sds((seq // BQ, 8, BQ), f32)]
    scratch = [pltpu.VMEM((2, d, HD), bf), pltpu.VMEM((2, HD, d), bf), pltpu.VMEM((2, d, HD), bf), pltpu.VMEM((2, HD, d), bf),
               pltpu.VMEM((4, rows, cols), bf), pltpu.VMEM((4, rows, width), bf), pltpu.VMEM((seq, width), bf),
               pltpu.VMEM((keys, 2 * HD), bf), pltpu.VMEM((HD, keys), bf), pltpu.VMEM((8, BQ), f32), pltpu.VMEM((8, BQ), f32),
               pltpu.VMEM((width, BQ), f32), pltpu.VMEM((2, BQ, width), bf),
               dma((5, nb)), dma((4, nb)), dma((n, 2)), dma((n, 2)), dma((n, 2)), dma((n, 2)), dma((n, 4)), dma((n, 4)),
               dma((2,)), dma((3,)), dma((nb,)), dma((nb, 3)), dma((4, nb)), dma((4,)), dma((4,)), dma((4, 2)), dma((4, 2)),
               dma((4,))]
    return pl.pallas_call(
        functools.partial(input_kernel, piece, keys // piece),
        out_shape=out_shape,
        in_specs=[vmem, vmem] + [hbm] * 4,
        out_specs=[hbm] * 6 + [vmem],
        scratch_shapes=scratch,
        name="input_phase",
        compiler_params=pltpu.CompilerParams(collective_id=1, has_side_effects=True, vmem_limit_bytes=VMEM),
        cost_estimate=pl.CostEstimate(flops=10 ** 11, bytes_accessed=10 ** 7, transcendentals=0))(x, dy, wq, wk, wv, wo)


def y_kernel(o_ref, w_ref, y_ref):
    acc = mm(o_ref[0], w_ref[0], NN)
    for g in range(1, o_ref.shape[0]):
        acc = acc + mm(o_ref[g], w_ref[g], NN)
    y_ref[...] = acc.astype(jnp.bfloat16)


def y_proj(o, wo):
    ng, rows, nq = o.shape
    d = wo.shape[2]
    bn = 512
    return pl.pallas_call(
        y_kernel, grid=(d // bn,),
        out_shape=jax.ShapeDtypeStruct((rows, d), jnp.bfloat16),
        in_specs=[pl.BlockSpec((ng, rows, nq), lambda j: (0, 0, 0)), pl.BlockSpec((ng, nq, bn), lambda j: (0, 0, j))],
        out_specs=pl.BlockSpec((rows, bn), lambda j: (0, j)),
        name="y_proj", compiler_params=pltpu.CompilerParams(vmem_limit_bytes=VMEM),
        cost_estimate=pl.CostEstimate(flops=2 * rows * d * nq * ng, bytes_accessed=30 * 10 ** 6, transcendentals=0))(o, wo)


def dx_kernel(dq_ref, dkv_ref, w_ref, dx_ref):
    nq = dq_ref.shape[2]
    acc = None
    for g in range(dq_ref.shape[0]):
        t = mm(dq_ref[g], w_ref[g, :, :nq], NT) + mm(dkv_ref[g], w_ref[g, :, nq:], NT)
        acc = t if acc is None else acc + t
    dx_ref[...] = acc.astype(jnp.bfloat16)


def dx_proj(dq, dkv, wqkv):
    ng, rows, nq = dq.shape
    _, d, cols = wqkv.shape
    bn = 512
    return pl.pallas_call(
        dx_kernel, grid=(d // bn,),
        out_shape=jax.ShapeDtypeStruct((rows, d), jnp.bfloat16),
        in_specs=[pl.BlockSpec((ng, rows, nq), lambda j: (0, 0, 0)), pl.BlockSpec((ng, rows, 2 * HD), lambda j: (0, 0, 0)),
                  pl.BlockSpec((ng, bn, cols), lambda j: (0, j, 0))],
        out_specs=pl.BlockSpec((rows, bn), lambda j: (0, j)),
        name="dx_proj", compiler_params=pltpu.CompilerParams(vmem_limit_bytes=VMEM),
        cost_estimate=pl.CostEstimate(flops=2 * rows * d * cols * ng, bytes_accessed=40 * 10 ** 6, transcendentals=0))(dq, dkv, wqkv)


def piece_row(j, piece, n_pieces):
    half = n_pieces // 2
    return jnp.where(j < half, j * 2 * piece, (n_pieces - 1 - j) * 2 * piece + piece)


def key_loop(n, piece, n_pieces, tile):
    per = piece // BQ
    full = n // per

    def whole(j, _):
        tile(pl.multiple_of(piece_row(j, piece, n_pieces), BQ), piece, False)
        return 0

    def part(j, _):
        tile(pl.multiple_of(piece_row(full, piece, n_pieces) + (j - full * per) * BQ, BQ), BQ, False)
        return 0

    lax.fori_loop(0, full, whole, 0)
    lax.fori_loop(full * per, n, part, 0)
    tile(pl.multiple_of(piece_row(full, piece, n_pieces) + (n - full * per) * BQ, BQ), BQ, True)


def keep_mask(size):
    r = lax.broadcasted_iota(jnp.int32, (size, BQ), 0)
    q = lax.broadcasted_iota(jnp.int32, (size, BQ), 1)
    return r <= q


def bwd_kernel(nh, piece, n_pieces, pos_ref, q_ref, do_ref, o_ref, lse_ref, kv_ref, dq_ref, dkv_ref, kt_ref, del_ref, dqt_ref):
    i = pl.program_id(0)
    n = pos_ref[i]

    @pl.when(i == 0)
    def _():
        dkv_ref[...] = jnp.zeros_like(dkv_ref)
        for b in range(n_pieces):
            kt_ref[:, b * piece:(b + 1) * piece] = kv_ref[b * piece:(b + 1) * piece, :HD].T

    for h in range(nh):
        sl = slice(h * HD, (h + 1) * HD)
        pr = do_ref[:, sl].astype(jnp.float32) * o_ref[:, sl].astype(jnp.float32)
        del_ref[h:h + 1, :] = jnp.sum(pr.T, axis=0, keepdims=True)
    dqt_ref[...] = jnp.zeros_like(dqt_ref)

    def tile(start, size, masked):
        for t0 in range(0, size, BQ):
            sub(start + t0, masked)

    def sub(start, masked):
        size = BQ
        k = kv_ref[pl.ds(start, size), :HD]
        v = kv_ref[pl.ds(start, size), HD:]
        kt = kt_ref[:, pl.ds(start, size)]
        dv = None
        dk = None
        for h in range(nh):
            sl = slice(h * HD, (h + 1) * HD)
            s = mm(k, q_ref[:, sl], NT) * (SCALE * LOG2E) - lse_ref[0, h:h + 1, :]
            dp = mm(v, do_ref[:, sl], NT)
            if masked:
                s = jnp.where(keep_mask(size), s, NEG)
            pb = jnp.exp2(s).astype(jnp.bfloat16)
            ds = (pb.astype(jnp.float32) * (dp - del_ref[h:h + 1, :])).astype(jnp.bfloat16)
            dvh = mm(pb, do_ref[:, sl], NN)
            dkh = mm(ds, q_ref[:, sl], NN)
            dv = dvh if dv is None else dv + dvh
            dk = dkh if dk is None else dk + dkh
            dqt_ref[sl, :] += mm(kt, ds, NN)
        dkv_ref[pl.ds(start, size), :HD] += dk * SCALE
        dkv_ref[pl.ds(start, size), HD:] += dv

    key_loop(n, piece, n_pieces, tile)
    for h in range(nh):
        sl = slice(h * HD, (h + 1) * HD)
        dq_ref[:, sl] = (dqt_ref[sl, :] * SCALE).T.astype(jnp.bfloat16)


def attn_bwd(pos, q, do, o, lse, kv, piece):
    rows, width = q.shape
    nh = width // HD
    keys = kv.shape[0]
    nq = rows // BQ
    row = pl.BlockSpec((BQ, width), lambda i, p: (i, 0))
    gs = pltpu.PrefetchScalarGridSpec(
        num_scalar_prefetch=1, grid=(nq,),
        in_specs=[row, row, row, pl.BlockSpec((1, 8, BQ), lambda i, p: (i, 0, 0)),
                  pl.BlockSpec((keys, 2 * HD), lambda i, p: (0, 0))],
        out_specs=[row, pl.BlockSpec((keys, 2 * HD), lambda i, p: (0, 0))],
        scratch_shapes=[pltpu.VMEM((HD, keys), jnp.bfloat16), pltpu.VMEM((8, BQ), jnp.float32),
                        pltpu.VMEM((width, BQ), jnp.float32)])
    return pl.pallas_call(
        functools.partial(bwd_kernel, nh, piece, keys // piece),
        out_shape=[jax.ShapeDtypeStruct(q.shape, jnp.bfloat16), jax.ShapeDtypeStruct((keys, 2 * HD), jnp.float32)],
        grid_spec=gs, name="attn_bwd", compiler_params=pltpu.CompilerParams(vmem_limit_bytes=VMEM),
        cost_estimate=pl.CostEstimate(flops=150 * 10 ** 9, bytes_accessed=10 ** 7, transcendentals=0))(pos, q, do, o, lse, kv)


def solution(mesh):
    cp_size = mesh.shape['cp']
    row_spec = P(('dp', 'cp', 'tp'), None)

    def local_step(x_blk, dy_blk, w_query, w_key, w_value, w_out):
        rows, d = x_blk.shape
        ng = mesh.shape['tp']
        seq_loc = rows * ng
        piece = seq_loc // 2
        width = w_query.shape[1]
        rank = lax.axis_index('cp')
        half = piece // BQ
        t = jnp.arange(2 * half, dtype=jnp.int32)
        pos = jnp.where(t < half, rank * half + t, (2 * cp_size - 1 - rank) * half + t - half).astype(jnp.int32)

        def a2a(v):
            return lax.all_to_all(v, 'tp', 0, 0, tiled=True)

        wqkv, wo, q_loc, kv_all, do_loc, o_loc, lse = input_phase(x_blk, dy_blk, w_query, w_key, w_value, w_out, cp_size)
        o_g = a2a(o_loc.reshape(ng, rows, width))
        dq_loc, dkv = attn_bwd(pos, q_loc, do_loc, o_loc, lse, kv_all, piece)
        y_blk = y_proj(o_g, wo)
        dq_g = a2a(dq_loc.reshape(ng, rows, width))
        dkv_own = lax.psum_scatter(dkv, 'cp', scatter_dimension=0, tiled=True).astype(jnp.bfloat16)
        dkv_g = a2a(dkv_own.reshape(ng, rows, 2 * HD))
        dx_blk = dx_proj(dq_g, dkv_g, wqkv)
        return y_blk, dx_blk

    return jax.shard_map(local_step, mesh=mesh, in_specs=(row_spec, row_spec, P(None, 'tp'), P(None, 'tp'), P(None, 'tp'), P('tp', None)),
                         out_specs=(row_spec, row_spec), check_vma=False)
```

```python
import functools
import jax
import jax.numpy as jnp
from jax import lax
from jax.experimental import pallas as pl
from jax.experimental.pallas import tpu as pltpu
from jax.sharding import PartitionSpec as P

HD = 128
BQ = 256
LOG2E = 1.4426950408889634
SCALE = HD ** -0.5
NT = (((1,), (1,)), ((), ()))
NN = (((1,), (0,)), ((), ()))
NEG = -1e30
VMEM = 60 * 2 ** 20
MESH_ID = pl.DeviceIdType.MESH


def mm(a, b, dims):
    return lax.dot_general(a, b, dims, preferred_element_type=jnp.float32)


def input_kernel(piece, n_pieces, x_ref, dy_ref, wq, wk, wv, wo, wqkv_all, wo_all, q_loc, kv_all, do_loc, o_loc, lse_ref,
                 wbuf, vbuf, obuf, pbuf, res, resd, qv, kvv, vt_ref, m_ref, l_ref, acc_ref, ost,
                 zs, zr, xs, xr, ys, yr, cs, cr, ls, os, orr, rs, rr, kys, kyr, kcs, kcr, fs):
    width = wq.shape[1]
    nh = width // HD
    nkv = nh + 2
    nb = nkv + nh
    n = 3 * nb
    x = lax.axis_index('dp')
    z = lax.axis_index('tp')
    cp = lax.axis_index('cp')
    y = cp // 2
    c = cp % 2
    hz = z // 2
    inner = jnp.logical_or(z == 1, z == 2)
    rows = x_ref.shape[0]
    dx = (1 - x, z, cp)
    dy = (x, z, (1 - y) * 2 + c)
    dc = (x, z, y * 2 + 1 - c)
    src = [1 - z + 4 * hz, 2 - hz, 3 - 3 * hz]

    def dz(s):
        return (x, s, cp)

    bar = pltpu.get_barrier_semaphore()
    for d in [dz(src[0]), dz(src[1]), dz(src[2]), dx, dy, dc]:
        pl.semaphore_signal(bar, inc=1, device_id=d, device_id_type=MESH_ID)
    pl.semaphore_wait(bar, 6)

    def eid(xx, yy, cc):
        return (xx * 2 + yy) * 2 + cc

    e0, ex, ey, ed = eid(x, y, c), eid(1 - x, y, c), eid(x, 1 - y, c), eid(1 - x, 1 - y, c)
    dk = wq.shape[0] // 8
    dr = HD // 8

    def by_kind(j, f):
        def qkv():
            f(True, pl.multiple_of(jnp.where(j < 2, width + j * HD, (j - 2) * HD), HD))

        def out():
            f(False, pl.multiple_of((j - nkv) * HD, HD))

        if isinstance(j, int):
            qkv() if j < nkv else out()
        else:
            pl.when(j < nkv)(qkv)
            pl.when(j >= nkv)(out)

    def block(qkv, s, off):
        return wqkv_all.at[s, :, pl.ds(off, HD)] if qkv else wo_all.at[s, pl.ds(off, HD), :]

    def eighth(qkv, s, e, off):
        if qkv:
            return wqkv_all.at[s, pl.ds(pl.multiple_of(e * dk, 16), dk), pl.ds(off, HD)]
        return wo_all.at[s, pl.ds(pl.multiple_of(off + e * dr, 16), dr), :]

    def own_block(j):
        if j < 2:
            return (wk, wv)[j], 0
        return (wq, (j - 2) * HD) if j < nkv else (wo, (j - nkv) * HD)

    def rc(a, b, ss, rsem, dev):
        return pltpu.make_async_remote_copy(src_ref=a, dst_ref=b, send_sem=ss, recv_sem=rsem, device_id=dev,
                                            device_id_type=MESH_ID)

    def own_piece(j):
        ref, off = own_block(j)
        if j < nkv:
            return ref.at[pl.ds(pl.multiple_of(e0 * dk, 16), dk), pl.ds(off, HD)]
        return ref.at[pl.ds(pl.multiple_of(off + e0 * dr, 16), dr), :]

    prim, sec = [], []
    for j in range(nb):
        dst = []
        by_kind(j, lambda qkv, off: dst.append(eighth(qkv, z, e0, off)))
        prim.append(rc(own_piece(j), dst[0], zs.at[0, j], zr.at[z, j], dz(src[0])))
        sec.append(rc(own_piece(j), dst[0], zs.at[1, j], zr.at[z, j], dz(3 - z)))

    def own_send(j0, j1):
        for q in prim[j0:j1]:
            q.start()

        @pl.when(inner)
        def _():
            for q in sec[j0:j1]:
                q.start()

    own_send(0, nkv)

    def unit(i):
        j, k = i // 3, i % 3
        return j, k, jnp.where(k == 0, src[0], jnp.where(k == 1, src[1], src[2]))

    def copies(i, qkv, off):
        j, k, s = unit(i)
        tgt = jnp.where(k == 0, 3 - z, (z - 1) * 3)
        un = functools.partial(eighth, qkv, s, off=off)
        d = dict(zr=rc(un(e0), un(e0), zs.at[2 + k, j], zr.at[s, j], dz(s)),
                 zf=rc(un(e0), un(e0), zs.at[2 + k, j], zr.at[s, j], dz(tgt)),
                 x=rc(un(e0), un(e0), xs.at[i, 0], xr.at[i, 0], dx),
                 y=rc(un(e0), un(e0), ys.at[i, 0], yr.at[i, 0], dy),
                 fy=rc(un(ex), un(ex), ys.at[i, 1], yr.at[i, 1], dy),
                 fx=rc(un(ey), un(ey), xs.at[i, 1], xr.at[i, 1], dx))
        for q, e in enumerate((e0, ex, ey, ed)):
            d[q] = rc(un(e), un(e), cs.at[i, q], cr.at[i, q], dc)
        return d

    def stage(i, f):
        def run(qkv, off):
            d = copies(i, qkv, off)
            pl.when(i % 2 == 0)(functools.partial(f, d, True))
            pl.when(i % 2 == 1)(functools.partial(f, d, False))

        @pl.when(jnp.logical_and(i >= 0, i < n))
        def _():
            by_kind(i // 3, run)

    def st1(d, even):
        d['zr'].wait_recv()

        @pl.when(inner)
        def _():
            d['zf'].start()

        d['x' if even else 'y'].start()
        d['y' if even else 'x'].start()
        d[0].start()

    def st2(d, even):
        d['x' if even else 'y'].wait_recv()
        d['fy' if even else 'fx'].start()
        d[1 if even else 2].start()

    def st3(d, even):
        d['y' if even else 'x'].wait_recv()
        d[2 if even else 1].start()

    def st4(d, even):
        d['fy' if even else 'fx'].wait_recv()
        d[3].start()

    def arow(t):
        return pl.ds(pl.multiple_of(t * rows, 16), rows)

    def kvrow(p, t):
        return pl.ds(pl.multiple_of((p * 4 + t) * rows, 16), rows)

    def project(qkv, buf, slot, off):
        step = rows // 3

        def part(r, _):
            w = pl.ds(pl.multiple_of(r * step, 16), step)
            if qkv:
                res[slot, w, pl.ds(off, HD)] = mm(x_ref[w, :], buf, NN).astype(jnp.bfloat16)
            else:
                resd[slot, w, pl.ds(off, HD)] = mm(dy_ref[w, :], buf, NT).astype(jnp.bfloat16)
            return 0

        lax.fori_loop(0, 3, part, 0)

    def result(j, slot, t, f):
        def run(qkv, off):
            here = (res if qkv else resd).at[slot, :, pl.ds(off, HD)]
            if not qkv:
                f(here, do_loc.at[arow(t), pl.ds(off, HD)])
                return

            @pl.when(j < 2)
            def _():
                f(here, kv_all.at[kvrow(cp, t), pl.ds(pl.multiple_of(j * HD, HD), HD)])

            @pl.when(j >= 2)
            def _():
                f(here, q_loc.at[arow(t), pl.ds(off, HD)])

        by_kind(j, run)

    def load(i, qkv, off):
        _, _, s = unit(i)
        return pltpu.make_async_copy(block(qkv, s, off), (wbuf if qkv else vbuf).at[i % 2], ls.at[i % 2])

    def st5(i):
        @pl.when(jnp.logical_and(i >= 0, i < n))
        def _():
            def run(qkv, off):
                d = copies(i, qkv, off)
                for q in range(4):
                    d[q].wait_recv()
                load(i, qkv, off).start()

            by_kind(i // 3, run)

    def st6(i):
        @pl.when(jnp.logical_and(i >= 0, i < n))
        def _():
            j, k, s = unit(i)

            def run(qkv, off):
                load(i, qkv, off).wait()
                project(qkv, (wbuf if qkv else vbuf)[i % 2], k, off)

            by_kind(j, run)
            result(j, k, z, lambda a, b: rc(a, b, rs.at[j, k], rr.at[z, j], dz(s)).start())

    def own_in(j, f):
        def run(qkv, off):
            buf = (obuf if qkv else pbuf).at[j % 2]
            if not qkv:
                f(pltpu.make_async_copy(wo.at[pl.ds(off, HD), :], buf, os.at[j % 2]))
            elif isinstance(j, int) and j < 2:
                f(pltpu.make_async_copy((wk, wv)[j], buf, os.at[j % 2]))
            else:
                f(pltpu.make_async_copy(wq.at[:, pl.ds(off, HD)], buf, os.at[j % 2]))

        by_kind(j, run)

    def own_do(j):
        own_in(j, lambda q: q.wait())

        def run(qkv, off):
            buf = (obuf if qkv else pbuf)
            keep = pltpu.make_async_copy(buf.at[j % 2], block(qkv, z, off), os.at[2])
            keep.start()
            project(qkv, buf[j % 2], 3, off)
            keep.wait()

        by_kind(j, run)
        result(j, 3, z, lambda a, b: pltpu.make_async_copy(a, b, orr.at[j]).start())

    def own_wait(j0, j1):
        for j in range(j0, j1):
            if j < 2:
                pltpu.make_async_copy(res.at[3, :, pl.ds(width + j * HD, HD)], kv_all.at[kvrow(cp, z), pl.ds(j * HD, HD)], orr.at[j]).wait()
            elif j < nkv:
                pltpu.make_async_copy(res.at[3, :, pl.ds((j - 2) * HD, HD)], q_loc.at[arow(z), pl.ds((j - 2) * HD, HD)], orr.at[j]).wait()
            else:
                o = (j - nkv) * HD
                pltpu.make_async_copy(resd.at[3, :, pl.ds(o, HD)], do_loc.at[arow(z), pl.ds(o, HD)], orr.at[j]).wait()

    def got(j0, j1):
        for j in range(j0, j1):
            for k in range(3):
                t = src[k]
                if j < 2:
                    a = kv_all.at[kvrow(cp, t), pl.ds(j * HD, HD)]
                elif j < nkv:
                    a = q_loc.at[arow(t), pl.ds((j - 2) * HD, HD)]
                else:
                    a = do_loc.at[arow(t), pl.ds((j - nkv) * HD, HD)]
                rc(a, a, rs.at[j, k], rr.at[t, j], dz(t)).wait_recv()

    py = (1 - y) * 2 + c
    ts = [z] + src
    kva = [kv_all.at[kvrow(cp, t), :] for t in ts]
    kvb = [kv_all.at[kvrow(py, t), :] for t in ts]
    kyc = [rc(a, a, kys.at[j], kyr.at[j], dy) for j, a in enumerate(kva)]
    kyg = [rc(a, a, kys.at[j], kyr.at[j], dy) for j, a in enumerate(kvb)]
    kcc = [rc(a, a, kcs.at[j, 0], kcr.at[j, 0], dc) for j, a in enumerate(kva)]
    kcf = [rc(a, a, kcs.at[j, 1], kcr.at[j, 1], dc) for j, a in enumerate(kvb)]

    def kv1(j):
        if j == 0:
            own_wait(0, 2)
        else:
            t = ts[j]
            for b in range(2):
                a = kv_all.at[kvrow(cp, t), pl.ds(b * HD, HD)]
                rc(a, a, rs.at[b, j - 1], rr.at[t, b], dz(t)).wait_recv()
        kyc[j].start()
        kcc[j].start()

    def kv2(j):
        kyg[j].wait_recv()
        kcf[j].start()

    per = piece // BQ
    n_units = per * (n_pieces + 1)
    load_q = pltpu.make_async_copy(q_loc, qv, fs.at[0])
    load_kv = pltpu.make_async_copy(kv_all, kvv, fs.at[1])

    def fwd_load():
        for j in range(4):
            kcc[j].wait_recv()
            kcf[j].wait_recv()
        load_kv.start()
        own_wait(2, nkv)
        got(2, nkv)
        load_q.start()
        load_kv.wait()
        for b in range(n_pieces):
            vt_ref[:, b * piece:(b + 1) * piece] = kvv[b * piece:(b + 1) * piece, HD:].T
        load_q.wait()

    def o_out(i):
        return pltpu.make_async_copy(ost.at[i % 2], o_loc.at[pl.ds(pl.multiple_of(i * BQ, BQ), BQ), :], fs.at[2 + i % 2])

    def fwd_unit(u):
        n0 = cp + 1
        n1 = n_pieces - cp
        early = u < per * n0
        v = u - per * n0
        i = jnp.where(early, u // n0, per + v // n1)
        j = jnp.where(early, u % n0, v % n1)
        diag = j == jnp.where(early, n0, n1) - 1
        start = pl.multiple_of(piece_row(j, piece, n_pieces), BQ)
        qrow = pl.ds(pl.multiple_of(i * BQ, BQ), BQ)

        @pl.when(j == 0)
        def _():
            m_ref[...] = jnp.full_like(m_ref, NEG)
            l_ref[...] = jnp.zeros_like(l_ref)
            acc_ref[...] = jnp.zeros_like(acc_ref)

        def tile(masked):
            k = kvv[pl.ds(start, piece), :HD]
            vt = vt_ref[:, pl.ds(start, piece)]
            if masked:
                kr = lax.broadcasted_iota(jnp.int32, (piece, BQ), 0)
                qr = lax.broadcasted_iota(jnp.int32, (piece, BQ), 1)
                keep = kr <= qr + (i % per) * BQ
            scores = [mm(k, qv[qrow, h * HD:(h + 1) * HD], NT) for h in range(nh)]
            for h in range(nh):
                s = scores[h] * (SCALE * LOG2E)
                if masked:
                    s = jnp.where(keep, s, NEG)
                m_old = m_ref[h:h + 1, :]
                m_new = jnp.maximum(m_old, jnp.max(s, axis=0, keepdims=True))
                p = jnp.exp2(s - m_new)
                a = jnp.exp2(m_old - m_new)
                m_ref[h:h + 1, :] = m_new
                l_ref[h:h + 1, :] = l_ref[h:h + 1, :] * a + jnp.sum(p, axis=0, keepdims=True)
                o = mm(vt, p.astype(jnp.bfloat16), NN)
                acc_ref[h * HD:(h + 1) * HD, :] = acc_ref[h * HD:(h + 1) * HD, :] * a + o

        @pl.when(jnp.logical_not(diag))
        def _():
            tile(False)

        @pl.when(diag)
        def _():
            tile(True)

            @pl.when(i >= 2)
            def _():
                o_out(i).wait()

            for h in range(nh):
                l = l_ref[h:h + 1, :]
                o = acc_ref[h * HD:(h + 1) * HD, :] / l
                ost[i % 2, :, h * HD:(h + 1) * HD] = o.T.astype(jnp.bfloat16)
                lse_ref[i, h:h + 1, :] = m_ref[h:h + 1, :] + jnp.log2(l)
            o_out(i).start()

    own_in(0, lambda q: q.start())
    own_in(1, lambda q: q.start())
    own_do(0)
    own_in(2, lambda q: q.start())
    own_do(1)

    f0 = 3 * nkv + FWD_AT
    f1 = n + 5

    def once(i, at, f, *args):
        pl.when(i == at)(functools.partial(f, *args))

    def step(i, _):
        stage(i, st1)
        stage(i - 1, st2)
        stage(i - 2, st3)
        stage(i - 3, st4)
        st6(i - 5)
        st5(i - 4)
        j = i // 3

        @pl.when(jnp.logical_and(i % 3 == 1, jnp.logical_and(j >= 2, j < nb)))
        def _():
            own_do(j)

        @pl.when(jnp.logical_and(i % 3 == 2, jnp.logical_and(j >= 2, j + 1 < nb)))
        def _():
            own_in(j + 1, lambda q: q.start())

        once(i, 2, kv1, 0)
        for k in range(1, 4):
            once(i, 9 + k, kv1, k)
        for k in range(4):
            once(i, 12 + k, kv2, k)
        once(i, 2 * nkv, own_send, nkv, nb)
        once(i, f0, fwd_load)

        @pl.when(i > f0)
        def _():
            lax.fori_loop(n_units * (i - 1 - f0) // (f1 - f0), n_units * (i - f0) // (f1 - f0), lambda u, _: (fwd_unit(u), 0)[1], 0)

        return 0

    lax.fori_loop(0, f1 + 1, step, 0)

    for i in range(2 * per - 2, 2 * per):
        o_out(i).wait()
    for q in prim:
        q.wait_send()

    @pl.when(inner)
    def _():
        for q in sec:
            q.wait_send()

    def drain(i, _):
        def f(d, even):
            @pl.when(inner)
            def _():
                d['zf'].wait_send()
            for q in ['x', 'y', 'fy' if even else 'fx', 0, 1, 2, 3]:
                d[q].wait_send()

        stage(i, f)
        j, k, s = unit(i)
        result(j, k, z, lambda a, b: rc(a, b, rs.at[j, k], rr.at[z, j], dz(s)).wait_send())
        return 0

    lax.fori_loop(0, n, drain, 0)
    own_wait(nkv, nb)
    got(nkv, nb)
    for j in range(4):
        kyc[j].wait_send()
        kcc[j].wait_send()
        kcf[j].wait_send()


FWD_AT = 9


def input_phase(x, dy, wq, wk, wv, wo, cp_size):
    rows, d = x.shape
    width = wq.shape[1]
    cols = width + 2 * HD
    nb = 2 * (width // HD) + 2
    n = 3 * nb
    seq = 4 * rows
    piece = seq // 2
    keys = seq * cp_size
    bf, f32 = jnp.bfloat16, jnp.float32
    dma = pltpu.SemaphoreType.DMA
    hbm = pl.BlockSpec(memory_space=pltpu.HBM)
    vmem = pl.BlockSpec(memory_space=pltpu.VMEM)
    sds = jax.ShapeDtypeStruct
    out_shape = [sds((4, d, cols), bf), sds((4, width, d), bf), sds((seq, width), bf), sds((keys, 2 * HD), bf),
                 sds((seq, width), bf), sds((seq, width), bf), sds((seq // BQ, 8, BQ), f32)]
    scratch = [pltpu.VMEM((2, d, HD), bf), pltpu.VMEM((2, HD, d), bf), pltpu.VMEM((2, d, HD), bf), pltpu.VMEM((2, HD, d), bf),
               pltpu.VMEM((4, rows, cols), bf), pltpu.VMEM((4, rows, width), bf), pltpu.VMEM((seq, width), bf),
               pltpu.VMEM((keys, 2 * HD), bf), pltpu.VMEM((HD, keys), bf), pltpu.VMEM((8, BQ), f32), pltpu.VMEM((8, BQ), f32),
               pltpu.VMEM((width, BQ), f32), pltpu.VMEM((2, BQ, width), bf),
               dma((5, nb)), dma((4, nb)), dma((n, 2)), dma((n, 2)), dma((n, 2)), dma((n, 2)), dma((n, 4)), dma((n, 4)),
               dma((2,)), dma((3,)), dma((nb,)), dma((nb, 3)), dma((4, nb)), dma((4,)), dma((4,)), dma((4, 2)), dma((4, 2)),
               dma((4,))]
    return pl.pallas_call(
        functools.partial(input_kernel, piece, keys // piece),
        out_shape=out_shape,
        in_specs=[vmem, vmem] + [hbm] * 4,
        out_specs=[hbm] * 6 + [vmem],
        scratch_shapes=scratch,
        name="input_phase",
        compiler_params=pltpu.CompilerParams(collective_id=1, has_side_effects=True, vmem_limit_bytes=VMEM),
        cost_estimate=pl.CostEstimate(flops=10 ** 11, bytes_accessed=10 ** 7, transcendentals=0))(x, dy, wq, wk, wv, wo)


def piece_row(j, piece, n_pieces):
    half = n_pieces // 2
    return jnp.where(j < half, j * 2 * piece, (n_pieces - 1 - j) * 2 * piece + piece)


def keep_mask(size):
    r = lax.broadcasted_iota(jnp.int32, (size, BQ), 0)
    q = lax.broadcasted_iota(jnp.int32, (size, BQ), 1)
    return r <= q


def output_kernel(piece, n_pieces, q_ref, do_ref, o_ref, lse_ref, kv_ref, wqkv, wo, y_ref, dx_ref,
                  kt_ref, del_ref, dqt_ref, dkv_ref, stg, og, dqg, dkg, cbuf, ybuf, fin, wob, wqb, wkb, acc, tile_out,
                  os, orr, qs, qr, cs, cr, ys, yr, ks, kr, ls, ts):
    width = q_ref.shape[1]
    nh = width // HD
    rows = og.shape[1]
    d = wo.shape[2]
    x = lax.axis_index('dp')
    z = lax.axis_index('tp')
    cp = lax.axis_index('cp')
    y = cp // 2
    c = cp % 2
    hz = z // 2
    src = [1 - z + 4 * hz, 2 - hz, 3 - 3 * hz]
    dy = (x, z, (1 - y) * 2 + c)
    dc = (x, z, y * 2 + 1 - c)

    def dz(s):
        return (x, s, cp)

    def rc(a, b, ss, rsem, dev):
        return pltpu.make_async_remote_copy(src_ref=a, dst_ref=b, send_sem=ss, recv_sem=rsem, device_id=dev,
                                            device_id_type=MESH_ID)

    bar = pltpu.get_barrier_semaphore()
    for dev in [dz(src[0]), dz(src[1]), dz(src[2]), dy, dc]:
        pl.semaphore_signal(bar, inc=1, device_id=dev, device_id_type=MESH_ID)
    pl.semaphore_wait(bar, 5)

    def arow(t):
        return pl.ds(pl.multiple_of(t * rows, 16), rows)

    osend = [rc(o_ref.at[arow(t), :], og.at[z], os.at[k], orr.at[z], dz(t)) for k, t in enumerate(src)]
    orecv = [rc(o_ref.at[arow(t), :], og.at[t], os.at[k], orr.at[t], dz(t)) for k, t in enumerate(src)]
    for q in osend:
        q.start()
    og[z] = o_ref[arow(z), :]

    per = piece // BQ
    half = BQ // 2
    dkv_ref[...] = jnp.zeros_like(dkv_ref)
    for b in range(n_pieces):
        kt_ref[:, b * piece:(b + 1) * piece] = kv_ref[b * piece:(b + 1) * piece, :HD].T

    def dq_send(i, u, f):
        r0 = i * BQ + u * half
        t = r0 // rows
        r = pl.multiple_of(r0 - t * rows, half)

        @pl.when(t != z)
        def _():
            f(rc(stg.at[i % 2, pl.ds(u * half, half), :], dqg.at[z, pl.ds(r, half), :], qs.at[i % 2, u],
                 qr.at[z, r // half], dz(t)))

    def query_tile(ii, _):
        i = (ii + per) % (2 * per)
        n = jnp.where(i < per, cp * per + i, (n_pieces - 1 - cp) * per + i - per)
        qrow = pl.ds(pl.multiple_of(i * BQ, BQ), BQ)
        for h in range(nh):
            sl = slice(h * HD, (h + 1) * HD)
            pr = do_ref[qrow, sl].astype(jnp.float32) * o_ref[qrow, sl].astype(jnp.float32)
            del_ref[h:h + 1, :] = jnp.sum(pr.T, axis=0, keepdims=True)
        dqt_ref[...] = jnp.zeros_like(dqt_ref)

        def sub(start, masked):
            krow = pl.ds(start, BQ)
            k = kv_ref[krow, :HD]
            v = kv_ref[krow, HD:]
            kt = kt_ref[:, krow]
            dv = None
            dk = None
            for h in range(nh):
                sl = slice(h * HD, (h + 1) * HD)
                q = q_ref[qrow, sl]
                do = do_ref[qrow, sl]
                s = mm(k, q, NT) * (SCALE * LOG2E) - lse_ref[i, h:h + 1, :]
                dp = mm(v, do, NT)
                if masked:
                    s = jnp.where(keep_mask(BQ), s, NEG)
                pb = jnp.exp2(s).astype(jnp.bfloat16)
                ds = (pb.astype(jnp.float32) * (dp - del_ref[h:h + 1, :])).astype(jnp.bfloat16)
                dvh = mm(pb, do, NN)
                dkh = mm(ds, q, NN)
                dv = dvh if dv is None else dv + dvh
                dk = dkh if dk is None else dk + dkh
                dqt_ref[sl, :] += mm(kt, ds, NN)
            dkv_ref[krow, :HD] += dk
            dkv_ref[krow, HD:] += dv

        full = n // per

        def whole(j, _):
            start = piece_row(j, piece, n_pieces)
            for t0 in range(0, piece, BQ):
                sub(pl.multiple_of(start + t0, BQ), False)
            return 0

        def part(j, _):
            sub(pl.multiple_of(piece_row(full, piece, n_pieces) + (j - full * per) * BQ, BQ), False)
            return 0

        lax.fori_loop(0, full, whole, 0)
        lax.fori_loop(full * per, n, part, 0)
        sub(pl.multiple_of(piece_row(full, piece, n_pieces) + (n - full * per) * BQ, BQ), True)

        @pl.when(ii >= 2)
        def _():
            for u in range(2):
                dq_send((ii - 2 + per) % (2 * per), u, lambda q: q.wait_send())

        for h in range(nh):
            sl = slice(h * HD, (h + 1) * HD)
            stg[i % 2, :, sl] = (dqt_ref[sl, :] * SCALE).T.astype(jnp.bfloat16)
        for u in range(2):
            dq_send(i, u, lambda q: q.start())
            r0 = i * BQ + u * half
            t = r0 // rows

            @pl.when(t == z)
            def _(u=u, r0=r0, t=t):
                dqg[z, pl.ds(pl.multiple_of(r0 - t * rows, half), half), :] = stg[i % 2, u * half:(u + 1) * half, :]

        return 0

    lax.fori_loop(0, 2 * per, query_tile, 0)

    seq = 2 * piece

    def kvblock(b):
        return pl.ds(pl.multiple_of(b * seq, BQ), seq)

    csend = [rc(dkv_ref.at[kvblock(2 * yy + 1 - c), :], cbuf.at[q], cs.at[q], cr.at[q], dc) for q, yy in enumerate((1 - y, y))]
    for q in csend:
        q.start()

    bn = wob.shape[3]
    nt = d // bn

    def load_o(j):
        return pltpu.make_async_copy(wo.at[:, :, pl.ds(pl.multiple_of(j * bn, bn), bn)], wob.at[j % 2], ls.at[j % 2])

    def load_q(j):
        return pltpu.make_async_copy(wqkv.at[:, pl.ds(pl.multiple_of(j * bn, bn), bn), pl.ds(0, width)], wqb.at[j % 2], ls.at[2 + j % 2])

    def load_kv(j):
        return pltpu.make_async_copy(wqkv.at[:, pl.ds(pl.multiple_of(j * bn, bn), bn), pl.ds(width, 2 * HD)], wkb.at[j % 2], ls.at[4 + j % 2])

    def store(ref, j):
        return pltpu.make_async_copy(tile_out.at[j % 2], ref.at[:, pl.ds(pl.multiple_of(j * bn, bn), bn)], ts.at[j % 2])

    load_o(0).start()
    load_o(1).start()
    csend[0].wait_recv()
    other = kvblock(2 * (1 - y) + c)
    dkv_ref[other, :] += cbuf[0]
    ysend = rc(dkv_ref.at[other, :], ybuf, ys, yr, dy)
    ysend.start()
    for q in orecv:
        q.wait_recv()

    def y_tile(j, _):
        load_o(j).wait()
        t = mm(og[0], wob[j % 2, 0], NN)
        for g in range(1, 4):
            t = t + mm(og[g], wob[j % 2, g], NN)

        @pl.when(j >= 2)
        def _():
            store(y_ref, j - 2).wait()

        tile_out[j % 2] = t.astype(jnp.bfloat16)
        store(y_ref, j).start()

        @pl.when(j + 2 < nt)
        def _():
            load_o(j + 2).start()

        return 0

    load_q(0).start()
    load_q(1).start()
    lax.fori_loop(0, nt, y_tile, 0)
    for j in range(nt - 2, nt):
        store(y_ref, j).wait()

    for k in range(3):
        for u in range(rows // half):
            a = dqg.at[src[k], pl.ds(u * half, half), :]
            rc(a, a, qs.at[0, 0], qr.at[src[k], u], dz(src[k])).wait_recv()

    def dxq_tile(j, _):
        load_q(j).wait()
        t = mm(dqg[0], wqb[j % 2, 0], NT)
        for g in range(1, 4):
            t = t + mm(dqg[g], wqb[j % 2, g], NT)
        acc[j] = t

        @pl.when(j + 2 < nt)
        def _():
            load_q(j + 2).start()

        return 0

    h0 = nt // 2
    lax.fori_loop(0, h0, dxq_tile, 0)

    csend[1].wait_recv()
    ysend.wait_recv()
    mine = kvblock(2 * y + c)
    tot = dkv_ref[mine, :] + cbuf[1] + ybuf[...]
    fin[:, :HD] = (tot[:, :HD] * SCALE).astype(jnp.bfloat16)
    fin[:, HD:] = tot[:, HD:].astype(jnp.bfloat16)
    ksend = [rc(fin.at[arow(t), :], dkg.at[z], ks.at[k], kr.at[z], dz(t)) for k, t in enumerate(src)]
    krecv = [rc(fin.at[arow(t), :], dkg.at[t], ks.at[k], kr.at[t], dz(t)) for k, t in enumerate(src)]
    for q in ksend:
        q.start()
    dkg[z] = fin[arow(z), :]
    load_kv(0).start()
    load_kv(1).start()
    lax.fori_loop(h0, nt, dxq_tile, 0)
    for q in krecv:
        q.wait_recv()

    def dx_tile(j, _):
        load_kv(j).wait()
        t = acc[j]
        for g in range(4):
            t = t + mm(dkg[g], wkb[j % 2, g], NT)

        @pl.when(j >= 2)
        def _():
            store(dx_ref, j - 2).wait()

        tile_out[j % 2] = t.astype(jnp.bfloat16)
        store(dx_ref, j).start()

        @pl.when(j + 2 < nt)
        def _():
            load_kv(j + 2).start()

        return 0

    lax.fori_loop(0, nt, dx_tile, 0)
    for j in range(nt - 2, nt):
        store(dx_ref, j).wait()
    for q in osend + csend + ksend + [ysend]:
        q.wait_send()
    for ii in range(2 * per - 2, 2 * per):
        for u in range(2):
            dq_send((ii + per) % (2 * per), u, lambda q: q.wait_send())


def output_phase(q, do, o, lse, kv, wqkv, wo):
    seq, width = q.shape
    keys = kv.shape[0]
    rows = seq // 4
    piece = seq // 2
    d = wo.shape[2]
    bn = 256
    nt = d // bn
    bf, f32 = jnp.bfloat16, jnp.float32
    dma = pltpu.SemaphoreType.DMA
    hbm = pl.BlockSpec(memory_space=pltpu.HBM)
    vmem = pl.BlockSpec(memory_space=pltpu.VMEM)
    v = pltpu.VMEM
    scratch = [v((HD, keys), bf), v((8, BQ), f32), v((width, BQ), f32), v((keys, 2 * HD), f32), v((2, BQ, width), bf),
               v((4, rows, width), bf), v((4, rows, width), bf), v((4, rows, 2 * HD), bf), v((2, seq, 2 * HD), f32),
               v((seq, 2 * HD), f32), v((seq, 2 * HD), bf), v((2, 4, width, bn), bf), v((2, 4, bn, width), bf),
               v((2, 4, bn, 2 * HD), bf), v((nt, rows, bn), f32), v((2, rows, bn), bf),
               dma((3,)), dma((4,)), dma((2, 2)), dma((4, 3)), dma((2,)), dma((2,)), dma, dma, dma((3,)), dma((4,)),
               dma((6,)), dma((2,))]
    return pl.pallas_call(
        functools.partial(output_kernel, piece, keys // piece),
        out_shape=[jax.ShapeDtypeStruct((rows, d), bf)] * 2,
        in_specs=[vmem] * 5 + [hbm] * 2,
        out_specs=[hbm] * 2,
        scratch_shapes=scratch,
        name="output_phase",
        compiler_params=pltpu.CompilerParams(collective_id=2, has_side_effects=True, vmem_limit_bytes=VMEM),
        cost_estimate=pl.CostEstimate(flops=10 ** 11, bytes_accessed=10 ** 7, transcendentals=0))(q, do, o, lse, kv, wqkv, wo)


def solution(mesh):
    cp_size = mesh.shape['cp']
    row_spec = P(('dp', 'cp', 'tp'), None)

    def local_step(x_blk, dy_blk, w_query, w_key, w_value, w_out):
        wqkv, wo, q, kv, do, o, lse = input_phase(x_blk, dy_blk, w_query, w_key, w_value, w_out, cp_size)
        return tuple(output_phase(q, do, o, lse, kv, wqkv, wo))

    return jax.shard_map(local_step, mesh=mesh, in_specs=(row_spec, row_spec, P(None, 'tp'), P(None, 'tp'), P(None, 'tp'), P('tp', None)),
                         out_specs=(row_spec, row_spec), check_vma=False)
```

```python
import functools
import jax
import jax.numpy as jnp
from jax import lax
from jax.experimental import pallas as pl
from jax.experimental.pallas import tpu as pltpu
from jax.sharding import PartitionSpec as P

HD = 128
BQ = 256
LOG2E = 1.4426950408889634
SCALE = HD ** -0.5
NT = (((1,), (1,)), ((), ()))
NN = (((1,), (0,)), ((), ()))
NEG = -1e30
VMEM = 60 * 2 ** 20
MESH_ID = pl.DeviceIdType.MESH


def mm(a, b, dims):
    return lax.dot_general(a, b, dims, preferred_element_type=jnp.float32)


def input_kernel(piece, n_pieces, x_ref, dy_ref, wq, wk, wv, wo, wqkv_all, wo_all, q_loc, kv_all, do_loc, o_loc, lse_ref,
                 wbuf, vbuf, obuf, pbuf, res, resd, qv, kvv, vt_ref, m_ref, l_ref, acc_ref, ost,
                 zs, zr, xs, xr, ys, yr, cs, cr, ls, os, orr, rs, rr, kys, kyr, kcs, kcr, fs):
    width = wq.shape[1]
    nh = width // HD
    nkv = nh + 2
    nb = nkv + nh
    n = 3 * nb
    x = lax.axis_index('dp')
    z = lax.axis_index('tp')
    cp = lax.axis_index('cp')
    y = cp // 2
    c = cp % 2
    hz = z // 2
    inner = jnp.logical_or(z == 1, z == 2)
    rows = x_ref.shape[0]
    dx = (1 - x, z, cp)
    dy = (x, z, (1 - y) * 2 + c)
    dc = (x, z, y * 2 + 1 - c)
    src = [1 - z + 4 * hz, 2 - hz, 3 - 3 * hz]

    def dz(s):
        return (x, s, cp)

    bar = pltpu.get_barrier_semaphore()
    for d in [dz(src[0]), dz(src[1]), dz(src[2]), dx, dy, dc]:
        pl.semaphore_signal(bar, inc=1, device_id=d, device_id_type=MESH_ID)
    pl.semaphore_wait(bar, 6)

    def eid(xx, yy, cc):
        return (xx * 2 + yy) * 2 + cc

    e0, ex, ey, ed = eid(x, y, c), eid(1 - x, y, c), eid(x, 1 - y, c), eid(1 - x, 1 - y, c)
    dk = wq.shape[0] // 8
    dr = HD // 8

    def by_kind(j, f):
        def qkv():
            f(True, pl.multiple_of(jnp.where(j < 2, width + j * HD, (j - 2) * HD), HD))

        def out():
            f(False, pl.multiple_of((j - nkv) * HD, HD))

        if isinstance(j, int):
            qkv() if j < nkv else out()
        else:
            pl.when(j < nkv)(qkv)
            pl.when(j >= nkv)(out)

    def block(qkv, s, off):
        return wqkv_all.at[s, :, pl.ds(off, HD)] if qkv else wo_all.at[s, pl.ds(off, HD), :]

    def eighth(qkv, s, e, off):
        if qkv:
            return wqkv_all.at[s, pl.ds(pl.multiple_of(e * dk, 16), dk), pl.ds(off, HD)]
        return wo_all.at[s, pl.ds(pl.multiple_of(off + e * dr, 16), dr), :]

    def own_block(j):
        if j < 2:
            return (wk, wv)[j], 0
        return (wq, (j - 2) * HD) if j < nkv else (wo, (j - nkv) * HD)

    def rc(a, b, ss, rsem, dev):
        return pltpu.make_async_remote_copy(src_ref=a, dst_ref=b, send_sem=ss, recv_sem=rsem, device_id=dev,
                                            device_id_type=MESH_ID)

    def own_piece(j):
        ref, off = own_block(j)
        if j < nkv:
            return ref.at[pl.ds(pl.multiple_of(e0 * dk, 16), dk), pl.ds(off, HD)]
        return ref.at[pl.ds(pl.multiple_of(off + e0 * dr, 16), dr), :]

    prim, sec = [], []
    for j in range(nb):
        dst = []
        by_kind(j, lambda qkv, off: dst.append(eighth(qkv, z, e0, off)))
        prim.append(rc(own_piece(j), dst[0], zs.at[0, j], zr.at[z, j], dz(src[0])))
        sec.append(rc(own_piece(j), dst[0], zs.at[1, j], zr.at[z, j], dz(3 - z)))

    def own_send(j0, j1):
        for q in prim[j0:j1]:
            q.start()

        @pl.when(inner)
        def _():
            for q in sec[j0:j1]:
                q.start()

    own_send(0, nkv)

    def unit(i):
        j, k = i // 3, i % 3
        return j, k, jnp.where(k == 0, src[0], jnp.where(k == 1, src[1], src[2]))

    def copies(i, qkv, off):
        j, k, s = unit(i)
        tgt = jnp.where(k == 0, 3 - z, (z - 1) * 3)
        un = functools.partial(eighth, qkv, s, off=off)
        d = dict(zr=rc(un(e0), un(e0), zs.at[2 + k, j], zr.at[s, j], dz(s)),
                 zf=rc(un(e0), un(e0), zs.at[2 + k, j], zr.at[s, j], dz(tgt)),
                 x=rc(un(e0), un(e0), xs.at[i, 0], xr.at[i, 0], dx),
                 y=rc(un(e0), un(e0), ys.at[i, 0], yr.at[i, 0], dy),
                 fy=rc(un(ex), un(ex), ys.at[i, 1], yr.at[i, 1], dy),
                 fx=rc(un(ey), un(ey), xs.at[i, 1], xr.at[i, 1], dx))
        for q, e in enumerate((e0, ex, ey, ed)):
            d[q] = rc(un(e), un(e), cs.at[i, q], cr.at[i, q], dc)
        return d

    def stage(i, f):
        def run(qkv, off):
            d = copies(i, qkv, off)
            pl.when(i % 2 == 0)(functools.partial(f, d, True))
            pl.when(i % 2 == 1)(functools.partial(f, d, False))

        @pl.when(jnp.logical_and(i >= 0, i < n))
        def _():
            by_kind(i // 3, run)

    def st1(d, even):
        d['zr'].wait_recv()

        @pl.when(inner)
        def _():
            d['zf'].start()

        d['x' if even else 'y'].start()
        d['y' if even else 'x'].start()
        d[0].start()

    def st2(d, even):
        d['x' if even else 'y'].wait_recv()
        d['fy' if even else 'fx'].start()
        d[1 if even else 2].start()

    def st3(d, even):
        d['y' if even else 'x'].wait_recv()
        d[2 if even else 1].start()

    def st4(d, even):
        d['fy' if even else 'fx'].wait_recv()
        d[3].start()

    def arow(t):
        return pl.ds(pl.multiple_of(t * rows, 16), rows)

    def kvrow(p, t):
        return pl.ds(pl.multiple_of((p * 4 + t) * rows, 16), rows)

    def project(qkv, buf, slot, off):
        step = rows // 3

        def part(r, _):
            w = pl.ds(pl.multiple_of(r * step, 16), step)
            if qkv:
                res[slot, w, pl.ds(off, HD)] = mm(x_ref[w, :], buf, NN).astype(jnp.bfloat16)
            else:
                resd[slot, w, pl.ds(off, HD)] = mm(dy_ref[w, :], buf, NT).astype(jnp.bfloat16)
            return 0

        lax.fori_loop(0, 3, part, 0)

    def result(j, slot, t, f):
        def run(qkv, off):
            here = (res if qkv else resd).at[slot, :, pl.ds(off, HD)]
            if not qkv:
                f(here, do_loc.at[arow(t), pl.ds(off, HD)])
                return

            @pl.when(j < 2)
            def _():
                f(here, kv_all.at[kvrow(cp, t), pl.ds(pl.multiple_of(j * HD, HD), HD)])

            @pl.when(j >= 2)
            def _():
                f(here, q_loc.at[arow(t), pl.ds(off, HD)])

        by_kind(j, run)

    def load(i, qkv, off):
        _, _, s = unit(i)
        return pltpu.make_async_copy(block(qkv, s, off), (wbuf if qkv else vbuf).at[i % 2], ls.at[i % 2])

    def st5(i):
        @pl.when(jnp.logical_and(i >= 0, i < n))
        def _():
            def run(qkv, off):
                d = copies(i, qkv, off)
                for q in range(4):
                    d[q].wait_recv()
                load(i, qkv, off).start()

            by_kind(i // 3, run)

    def st6(i):
        @pl.when(jnp.logical_and(i >= 0, i < n))
        def _():
            j, k, s = unit(i)

            def run(qkv, off):
                load(i, qkv, off).wait()
                project(qkv, (wbuf if qkv else vbuf)[i % 2], k, off)

            by_kind(j, run)
            result(j, k, z, lambda a, b: rc(a, b, rs.at[j, k], rr.at[z, j], dz(s)).start())

    def own_in(j, f):
        def run(qkv, off):
            buf = (obuf if qkv else pbuf).at[j % 2]
            if not qkv:
                f(pltpu.make_async_copy(wo.at[pl.ds(off, HD), :], buf, os.at[j % 2]))
            elif isinstance(j, int) and j < 2:
                f(pltpu.make_async_copy((wk, wv)[j], buf, os.at[j % 2]))
            else:
                f(pltpu.make_async_copy(wq.at[:, pl.ds(off, HD)], buf, os.at[j % 2]))

        by_kind(j, run)

    def own_do(j):
        own_in(j, lambda q: q.wait())

        def run(qkv, off):
            buf = (obuf if qkv else pbuf)
            keep = pltpu.make_async_copy(buf.at[j % 2], block(qkv, z, off), os.at[2])
            keep.start()
            project(qkv, buf[j % 2], 3, off)
            keep.wait()

        by_kind(j, run)
        result(j, 3, z, lambda a, b: pltpu.make_async_copy(a, b, orr.at[j]).start())

    def own_wait(j0, j1):
        for j in range(j0, j1):
            if j < 2:
                pltpu.make_async_copy(res.at[3, :, pl.ds(width + j * HD, HD)], kv_all.at[kvrow(cp, z), pl.ds(j * HD, HD)], orr.at[j]).wait()
            elif j < nkv:
                pltpu.make_async_copy(res.at[3, :, pl.ds((j - 2) * HD, HD)], q_loc.at[arow(z), pl.ds((j - 2) * HD, HD)], orr.at[j]).wait()
            else:
                o = (j - nkv) * HD
                pltpu.make_async_copy(resd.at[3, :, pl.ds(o, HD)], do_loc.at[arow(z), pl.ds(o, HD)], orr.at[j]).wait()

    def got(j0, j1):
        for j in range(j0, j1):
            for k in range(3):
                t = src[k]
                if j < 2:
                    a = kv_all.at[kvrow(cp, t), pl.ds(j * HD, HD)]
                elif j < nkv:
                    a = q_loc.at[arow(t), pl.ds((j - 2) * HD, HD)]
                else:
                    a = do_loc.at[arow(t), pl.ds((j - nkv) * HD, HD)]
                rc(a, a, rs.at[j, k], rr.at[t, j], dz(t)).wait_recv()

    py = (1 - y) * 2 + c
    ts = [z] + src
    kva = [kv_all.at[kvrow(cp, t), :] for t in ts]
    kvb = [kv_all.at[kvrow(py, t), :] for t in ts]
    kyc = [rc(a, a, kys.at[j], kyr.at[j], dy) for j, a in enumerate(kva)]
    kyg = [rc(a, a, kys.at[j], kyr.at[j], dy) for j, a in enumerate(kvb)]
    kcc = [rc(a, a, kcs.at[j, 0], kcr.at[j, 0], dc) for j, a in enumerate(kva)]
    kcf = [rc(a, a, kcs.at[j, 1], kcr.at[j, 1], dc) for j, a in enumerate(kvb)]

    def kv1(j):
        if j == 0:
            own_wait(0, 2)
        else:
            t = ts[j]
            for b in range(2):
                a = kv_all.at[kvrow(cp, t), pl.ds(b * HD, HD)]
                rc(a, a, rs.at[b, j - 1], rr.at[t, b], dz(t)).wait_recv()
        kyc[j].start()
        kcc[j].start()

    def kv2(j):
        kyg[j].wait_recv()
        kcf[j].start()

    per = piece // BQ
    n_units = per * (n_pieces + 1)
    load_q = pltpu.make_async_copy(q_loc, qv, fs.at[0])
    load_kv = pltpu.make_async_copy(kv_all, kvv, fs.at[1])

    def fwd_load():
        for j in range(4):
            kcc[j].wait_recv()
            kcf[j].wait_recv()
        load_kv.start()
        own_wait(2, nkv)
        got(2, nkv)
        load_q.start()
        load_kv.wait()
        for b in range(n_pieces):
            vt_ref[:, b * piece:(b + 1) * piece] = kvv[b * piece:(b + 1) * piece, HD:].T
        load_q.wait()

    def o_out(i):
        return pltpu.make_async_copy(ost.at[i % 2], o_loc.at[pl.ds(pl.multiple_of(i * BQ, BQ), BQ), :], fs.at[2 + i % 2])

    def fwd_unit(u):
        n0 = cp + 1
        n1 = n_pieces - cp
        early = u < per * n0
        v = u - per * n0
        i = jnp.where(early, u // n0, per + v // n1)
        j = jnp.where(early, u % n0, v % n1)
        diag = j == jnp.where(early, n0, n1) - 1
        start = pl.multiple_of(piece_row(j, piece, n_pieces), BQ)
        qrow = pl.ds(pl.multiple_of(i * BQ, BQ), BQ)

        @pl.when(j == 0)
        def _():
            m_ref[...] = jnp.full_like(m_ref, NEG)
            l_ref[...] = jnp.zeros_like(l_ref)
            acc_ref[...] = jnp.zeros_like(acc_ref)

        def tile(masked):
            k = kvv[pl.ds(start, piece), :HD]
            vt = vt_ref[:, pl.ds(start, piece)]
            if masked:
                kr = lax.broadcasted_iota(jnp.int32, (piece, BQ), 0)
                qr = lax.broadcasted_iota(jnp.int32, (piece, BQ), 1)
                keep = kr <= qr + (i % per) * BQ
            scores = [mm(k, qv[qrow, h * HD:(h + 1) * HD], NT) for h in range(nh)]
            for h in range(nh):
                s = scores[h]
                if masked:
                    s = jnp.where(keep, s, NEG)
                m_old = m_ref[h:h + 1, :]
                m_new = jnp.maximum(m_old, jnp.max(s, axis=0, keepdims=True) * (SCALE * LOG2E))
                p = jnp.exp2(s * (SCALE * LOG2E) - m_new)
                a = jnp.exp2(m_old - m_new)
                m_ref[h:h + 1, :] = m_new
                l_ref[h:h + 1, :] = l_ref[h:h + 1, :] * a + jnp.sum(p, axis=0, keepdims=True)
                o = mm(vt, p.astype(jnp.bfloat16), NN)
                acc_ref[h * HD:(h + 1) * HD, :] = acc_ref[h * HD:(h + 1) * HD, :] * a + o

        @pl.when(jnp.logical_not(diag))
        def _():
            tile(False)

        @pl.when(diag)
        def _():
            tile(True)

            @pl.when(i >= 2)
            def _():
                o_out(i).wait()

            for h in range(nh):
                l = l_ref[h:h + 1, :]
                o = acc_ref[h * HD:(h + 1) * HD, :] / l
                ost[i % 2, :, h * HD:(h + 1) * HD] = o.T.astype(jnp.bfloat16)
                lse_ref[i, h:h + 1, :] = m_ref[h:h + 1, :] + jnp.log2(l)
            o_out(i).start()

    own_in(0, lambda q: q.start())
    own_in(1, lambda q: q.start())
    own_do(0)
    own_in(2, lambda q: q.start())
    own_do(1)

    f0 = 3 * nkv + FWD_AT
    f1 = n + 5

    def once(i, at, f, *args):
        pl.when(i == at)(functools.partial(f, *args))

    def step(i, _):
        stage(i, st1)
        stage(i - 1, st2)
        stage(i - 2, st3)
        stage(i - 3, st4)
        st6(i - 5)
        st5(i - 4)
        j = i // 3

        @pl.when(jnp.logical_and(i % 3 == 1, jnp.logical_and(j >= 2, j < nb)))
        def _():
            own_do(j)

        @pl.when(jnp.logical_and(i % 3 == 2, jnp.logical_and(j >= 2, j + 1 < nb)))
        def _():
            own_in(j + 1, lambda q: q.start())

        once(i, 2, kv1, 0)
        for k in range(1, 4):
            once(i, 9 + k, kv1, k)
        for k in range(4):
            once(i, 12 + k, kv2, k)
        once(i, 2 * nkv, own_send, nkv, nb)
        once(i, f0, fwd_load)

        @pl.when(i > f0)
        def _():
            lax.fori_loop(n_units * (i - 1 - f0) // (f1 - f0), n_units * (i - f0) // (f1 - f0), lambda u, _: (fwd_unit(u), 0)[1], 0)

        return 0

    lax.fori_loop(0, f1 + 1, step, 0)

    for i in range(2 * per - 2, 2 * per):
        o_out(i).wait()
    for q in prim:
        q.wait_send()

    @pl.when(inner)
    def _():
        for q in sec:
            q.wait_send()

    def drain(i, _):
        def f(d, even):
            @pl.when(inner)
            def _():
                d['zf'].wait_send()
            for q in ['x', 'y', 'fy' if even else 'fx', 0, 1, 2, 3]:
                d[q].wait_send()

        stage(i, f)
        j, k, s = unit(i)
        result(j, k, z, lambda a, b: rc(a, b, rs.at[j, k], rr.at[z, j], dz(s)).wait_send())
        return 0

    lax.fori_loop(0, n, drain, 0)
    own_wait(nkv, nb)
    got(nkv, nb)
    for j in range(4):
        kyc[j].wait_send()
        kcc[j].wait_send()
        kcf[j].wait_send()


FWD_AT = 5


def input_phase(x, dy, wq, wk, wv, wo, cp_size):
    rows, d = x.shape
    width = wq.shape[1]
    cols = width + 2 * HD
    nb = 2 * (width // HD) + 2
    n = 3 * nb
    seq = 4 * rows
    piece = seq // 2
    keys = seq * cp_size
    bf, f32 = jnp.bfloat16, jnp.float32
    dma = pltpu.SemaphoreType.DMA
    hbm = pl.BlockSpec(memory_space=pltpu.HBM)
    vmem = pl.BlockSpec(memory_space=pltpu.VMEM)
    sds = jax.ShapeDtypeStruct
    out_shape = [sds((4, d, cols), bf), sds((4, width, d), bf), sds((seq, width), bf), sds((keys, 2 * HD), bf),
                 sds((seq, width), bf), sds((seq, width), bf), sds((seq // BQ, 8, BQ), f32)]
    scratch = [pltpu.VMEM((2, d, HD), bf), pltpu.VMEM((2, HD, d), bf), pltpu.VMEM((2, d, HD), bf), pltpu.VMEM((2, HD, d), bf),
               pltpu.VMEM((4, rows, cols), bf), pltpu.VMEM((4, rows, width), bf), pltpu.VMEM((seq, width), bf),
               pltpu.VMEM((keys, 2 * HD), bf), pltpu.VMEM((HD, keys), bf), pltpu.VMEM((8, BQ), f32), pltpu.VMEM((8, BQ), f32),
               pltpu.VMEM((width, BQ), f32), pltpu.VMEM((2, BQ, width), bf),
               dma((5, nb)), dma((4, nb)), dma((n, 2)), dma((n, 2)), dma((n, 2)), dma((n, 2)), dma((n, 4)), dma((n, 4)),
               dma((2,)), dma((3,)), dma((nb,)), dma((nb, 3)), dma((4, nb)), dma((4,)), dma((4,)), dma((4, 2)), dma((4, 2)),
               dma((4,))]
    return pl.pallas_call(
        functools.partial(input_kernel, piece, keys // piece),
        out_shape=out_shape,
        in_specs=[vmem, vmem] + [hbm] * 4,
        out_specs=[hbm] * 6 + [vmem],
        scratch_shapes=scratch,
        name="input_phase",
        compiler_params=pltpu.CompilerParams(collective_id=1, has_side_effects=True, vmem_limit_bytes=VMEM),
        cost_estimate=pl.CostEstimate(flops=10 ** 11, bytes_accessed=10 ** 7, transcendentals=0))(x, dy, wq, wk, wv, wo)


def piece_row(j, piece, n_pieces):
    half = n_pieces // 2
    return jnp.where(j < half, j * 2 * piece, (n_pieces - 1 - j) * 2 * piece + piece)


def keep_mask(size):
    r = lax.broadcasted_iota(jnp.int32, (size, BQ), 0)
    q = lax.broadcasted_iota(jnp.int32, (size, BQ), 1)
    return r <= q


def output_kernel(piece, n_pieces, q_ref, do_ref, o_ref, lse_ref, kv_ref, wqkv, wo, y_ref, dx_ref,
                  kt_ref, del_ref, dqt_ref, dkv_ref, stg, og, dqg, dkg, cbuf, ybuf, fin, wob, wqb, wkb, acc, tile_out,
                  os, orr, qs, qr, cs, cr, ys, yr, ks, kr, ls, ts):
    width = q_ref.shape[1]
    nh = width // HD
    rows = og.shape[1]
    d = wo.shape[2]
    x = lax.axis_index('dp')
    z = lax.axis_index('tp')
    cp = lax.axis_index('cp')
    y = cp // 2
    c = cp % 2
    hz = z // 2
    src = [1 - z + 4 * hz, 2 - hz, 3 - 3 * hz]
    dy = (x, z, (1 - y) * 2 + c)
    dc = (x, z, y * 2 + 1 - c)

    def dz(s):
        return (x, s, cp)

    def rc(a, b, ss, rsem, dev):
        return pltpu.make_async_remote_copy(src_ref=a, dst_ref=b, send_sem=ss, recv_sem=rsem, device_id=dev,
                                            device_id_type=MESH_ID)

    bar = pltpu.get_barrier_semaphore()
    for dev in [dz(src[0]), dz(src[1]), dz(src[2]), dy, dc]:
        pl.semaphore_signal(bar, inc=1, device_id=dev, device_id_type=MESH_ID)
    pl.semaphore_wait(bar, 5)

    def arow(t):
        return pl.ds(pl.multiple_of(t * rows, 16), rows)

    osend = [rc(o_ref.at[arow(t), :], og.at[z], os.at[k], orr.at[z], dz(t)) for k, t in enumerate(src)]
    orecv = [rc(o_ref.at[arow(t), :], og.at[t], os.at[k], orr.at[t], dz(t)) for k, t in enumerate(src)]
    for q in osend:
        q.start()
    og[z] = o_ref[arow(z), :]

    per = piece // BQ
    half = BQ // 2
    dkv_ref[...] = jnp.zeros_like(dkv_ref)
    for b in range(n_pieces):
        kt_ref[:, b * piece:(b + 1) * piece] = kv_ref[b * piece:(b + 1) * piece, :HD].T

    def dq_send(i, u, f):
        r0 = i * BQ + u * half
        t = r0 // rows
        r = pl.multiple_of(r0 - t * rows, half)

        @pl.when(t != z)
        def _():
            f(rc(stg.at[i % 2, pl.ds(u * half, half), :], dqg.at[z, pl.ds(r, half), :], qs.at[i % 2, u],
                 qr.at[z, r // half], dz(t)))

    def query_tile(ii, _):
        i = (ii + per) % (2 * per)
        n = jnp.where(i < per, cp * per + i, (n_pieces - 1 - cp) * per + i - per)
        qrow = pl.ds(pl.multiple_of(i * BQ, BQ), BQ)
        for h in range(nh):
            sl = slice(h * HD, (h + 1) * HD)
            pr = do_ref[qrow, sl].astype(jnp.float32) * o_ref[qrow, sl].astype(jnp.float32)
            del_ref[h:h + 1, :] = jnp.sum(pr.T, axis=0, keepdims=True)
        dqt_ref[...] = jnp.zeros_like(dqt_ref)

        def sub(start, size, masked):
            krow = pl.ds(start, size)
            k = kv_ref[krow, :HD]
            v = kv_ref[krow, HD:]
            kt = kt_ref[:, krow]

            def front(h):
                sl = slice(h * HD, (h + 1) * HD)
                return mm(k, q_ref[qrow, sl], NT), mm(v, do_ref[qrow, sl], NT)

            def back(h, pb, ds, dk, dv):
                sl = slice(h * HD, (h + 1) * HD)
                dvh = mm(pb, do_ref[qrow, sl], NN)
                dkh = mm(ds, q_ref[qrow, sl], NN)
                dqt_ref[sl, :] += mm(kt, ds, NN)
                return (dkh, dvh) if dk is None else (dk + dkh, dv + dvh)

            nxt = front(0)
            prev = None
            dk = dv = None
            for h in range(nh):
                s, dp = nxt
                if h + 1 < nh:
                    nxt = front(h + 1)
                if prev is not None:
                    dk, dv = back(*prev, dk, dv)
                s = s * (SCALE * LOG2E) - lse_ref[i, h:h + 1, :]
                if masked:
                    s = jnp.where(keep_mask(size), s, NEG)
                pb = jnp.exp2(s).astype(jnp.bfloat16)
                ds = (pb.astype(jnp.float32) * (dp - del_ref[h:h + 1, :])).astype(jnp.bfloat16)
                prev = (h, pb, ds)
            dk, dv = back(*prev, dk, dv)
            dkv_ref[krow, :HD] += dk
            dkv_ref[krow, HD:] += dv

        full = n // per

        def whole(j, _):
            sub(pl.multiple_of(piece_row(j, piece, n_pieces), BQ), piece, False)
            return 0

        def part(j, _):
            sub(pl.multiple_of(piece_row(full, piece, n_pieces) + (j - full * per) * BQ, BQ), BQ, False)
            return 0

        lax.fori_loop(0, full, whole, 0)
        lax.fori_loop(full * per, n, part, 0)
        sub(pl.multiple_of(piece_row(full, piece, n_pieces) + (n - full * per) * BQ, BQ), BQ, True)

        @pl.when(ii >= 2)
        def _():
            for u in range(2):
                dq_send((ii - 2 + per) % (2 * per), u, lambda q: q.wait_send())

        for h in range(nh):
            sl = slice(h * HD, (h + 1) * HD)
            stg[i % 2, :, sl] = (dqt_ref[sl, :] * SCALE).T.astype(jnp.bfloat16)
        for u in range(2):
            dq_send(i, u, lambda q: q.start())
            r0 = i * BQ + u * half
            t = r0 // rows

            @pl.when(t == z)
            def _(u=u, r0=r0, t=t):
                dqg[z, pl.ds(pl.multiple_of(r0 - t * rows, half), half), :] = stg[i % 2, u * half:(u + 1) * half, :]

        return 0

    lax.fori_loop(0, 2 * per, query_tile, 0)

    seq = 2 * piece

    def kvblock(b):
        return pl.ds(pl.multiple_of(b * seq, BQ), seq)

    csend = [rc(dkv_ref.at[kvblock(2 * yy + 1 - c), :], cbuf.at[q], cs.at[q], cr.at[q], dc) for q, yy in enumerate((1 - y, y))]
    for q in csend:
        q.start()

    bn = wob.shape[3]
    nt = d // bn

    def load_o(j):
        return pltpu.make_async_copy(wo.at[:, :, pl.ds(pl.multiple_of(j * bn, bn), bn)], wob.at[j % 2], ls.at[j % 2])

    def load_q(j):
        return pltpu.make_async_copy(wqkv.at[:, pl.ds(pl.multiple_of(j * bn, bn), bn), pl.ds(0, width)], wqb.at[j % 2], ls.at[2 + j % 2])

    def load_kv(j):
        return pltpu.make_async_copy(wqkv.at[:, pl.ds(pl.multiple_of(j * bn, bn), bn), pl.ds(width, 2 * HD)], wkb.at[j % 2], ls.at[4 + j % 2])

    def store(ref, j):
        return pltpu.make_async_copy(tile_out.at[j % 2], ref.at[:, pl.ds(pl.multiple_of(j * bn, bn), bn)], ts.at[j % 2])

    load_o(0).start()
    load_o(1).start()
    csend[0].wait_recv()
    other = kvblock(2 * (1 - y) + c)
    dkv_ref[other, :] += cbuf[0]
    ysend = rc(dkv_ref.at[other, :], ybuf, ys, yr, dy)
    ysend.start()
    for q in orecv:
        q.wait_recv()

    def y_tile(j, _):
        load_o(j).wait()
        t = mm(og[0], wob[j % 2, 0], NN)
        for g in range(1, 4):
            t = t + mm(og[g], wob[j % 2, g], NN)

        @pl.when(j >= 2)
        def _():
            store(y_ref, j - 2).wait()

        tile_out[j % 2] = t.astype(jnp.bfloat16)
        store(y_ref, j).start()

        @pl.when(j + 2 < nt)
        def _():
            load_o(j + 2).start()

        return 0

    load_q(0).start()
    load_q(1).start()
    lax.fori_loop(0, nt, y_tile, 0)
    for j in range(nt - 2, nt):
        store(y_ref, j).wait()

    for k in range(3):
        for u in range(rows // half):
            a = dqg.at[src[k], pl.ds(u * half, half), :]
            rc(a, a, qs.at[0, 0], qr.at[src[k], u], dz(src[k])).wait_recv()

    def dxq_tile(j, _):
        load_q(j).wait()
        t = mm(dqg[0], wqb[j % 2, 0], NT)
        for g in range(1, 4):
            t = t + mm(dqg[g], wqb[j % 2, g], NT)
        acc[j] = t

        @pl.when(j + 2 < nt)
        def _():
            load_q(j + 2).start()

        return 0

    h0 = nt // 2
    lax.fori_loop(0, h0, dxq_tile, 0)

    csend[1].wait_recv()
    ysend.wait_recv()
    mine = kvblock(2 * y + c)
    tot = dkv_ref[mine, :] + cbuf[1] + ybuf[...]
    fin[:, :HD] = (tot[:, :HD] * SCALE).astype(jnp.bfloat16)
    fin[:, HD:] = tot[:, HD:].astype(jnp.bfloat16)
    ksend = [rc(fin.at[arow(t), :], dkg.at[z], ks.at[k], kr.at[z], dz(t)) for k, t in enumerate(src)]
    krecv = [rc(fin.at[arow(t), :], dkg.at[t], ks.at[k], kr.at[t], dz(t)) for k, t in enumerate(src)]
    for q in ksend:
        q.start()
    dkg[z] = fin[arow(z), :]
    load_kv(0).start()
    load_kv(1).start()
    lax.fori_loop(h0, nt, dxq_tile, 0)
    for q in krecv:
        q.wait_recv()

    def dx_tile(j, _):
        load_kv(j).wait()
        t = acc[j]
        for g in range(4):
            t = t + mm(dkg[g], wkb[j % 2, g], NT)

        @pl.when(j >= 2)
        def _():
            store(dx_ref, j - 2).wait()

        tile_out[j % 2] = t.astype(jnp.bfloat16)
        store(dx_ref, j).start()

        @pl.when(j + 2 < nt)
        def _():
            load_kv(j + 2).start()

        return 0

    lax.fori_loop(0, nt, dx_tile, 0)
    for j in range(nt - 2, nt):
        store(dx_ref, j).wait()
    for q in osend + csend + ksend + [ysend]:
        q.wait_send()
    for ii in range(2 * per - 2, 2 * per):
        for u in range(2):
            dq_send((ii + per) % (2 * per), u, lambda q: q.wait_send())


def output_phase(q, do, o, lse, kv, wqkv, wo):
    seq, width = q.shape
    keys = kv.shape[0]
    rows = seq // 4
    piece = seq // 2
    d = wo.shape[2]
    bn = 256
    nt = d // bn
    bf, f32 = jnp.bfloat16, jnp.float32
    dma = pltpu.SemaphoreType.DMA
    hbm = pl.BlockSpec(memory_space=pltpu.HBM)
    vmem = pl.BlockSpec(memory_space=pltpu.VMEM)
    v = pltpu.VMEM
    scratch = [v((HD, keys), bf), v((8, BQ), f32), v((width, BQ), f32), v((keys, 2 * HD), f32), v((2, BQ, width), bf),
               v((4, rows, width), bf), v((4, rows, width), bf), v((4, rows, 2 * HD), bf), v((2, seq, 2 * HD), f32),
               v((seq, 2 * HD), f32), v((seq, 2 * HD), bf), v((2, 4, width, bn), bf), v((2, 4, bn, width), bf),
               v((2, 4, bn, 2 * HD), bf), v((nt, rows, bn), f32), v((2, rows, bn), bf),
               dma((3,)), dma((4,)), dma((2, 2)), dma((4, 3)), dma((2,)), dma((2,)), dma, dma, dma((3,)), dma((4,)),
               dma((6,)), dma((2,))]
    return pl.pallas_call(
        functools.partial(output_kernel, piece, keys // piece),
        out_shape=[jax.ShapeDtypeStruct((rows, d), bf)] * 2,
        in_specs=[vmem] * 5 + [hbm] * 2,
        out_specs=[hbm] * 2,
        scratch_shapes=scratch,
        name="output_phase",
        compiler_params=pltpu.CompilerParams(collective_id=2, has_side_effects=True, vmem_limit_bytes=VMEM),
        cost_estimate=pl.CostEstimate(flops=10 ** 11, bytes_accessed=10 ** 7, transcendentals=0))(q, do, o, lse, kv, wqkv, wo)


def solution(mesh):
    cp_size = mesh.shape['cp']
    row_spec = P(('dp', 'cp', 'tp'), None)

    def local_step(x_blk, dy_blk, w_query, w_key, w_value, w_out):
        wqkv, wo, q, kv, do, o, lse = input_phase(x_blk, dy_blk, w_query, w_key, w_value, w_out, cp_size)
        return tuple(output_phase(q, do, o, lse, kv, wqkv, wo))

    return jax.shard_map(local_step, mesh=mesh, in_specs=(row_spec, row_spec, P(None, 'tp'), P(None, 'tp'), P(None, 'tp'), P('tp', None)),
                         out_specs=(row_spec, row_spec), check_vma=False)
```
